32 devices in a mesh: tm: 8 (over z, y), env: 4 (over x, core).
Axes of the slice: x: 2, y: 2, z: 4, core: 2. Of those that a mesh axis runs over, the one named last changes fastest.
Arguments:
- rewards: float32 [16384, 2048], P('tm', 'env'), may hold values from -0.16 to 0.16
- values: float32 [16384, 2048], P('tm', 'env'), may hold values from -6 to 6
- last_value: float32 [2048], P('env'), may hold values from -6 to 6
- done_steps: int32 [2048, 4], P('env'), may hold values from 0 to 16383
- horizon_offset: int32 [2048], P('env'), may hold values from 0 to 8191
- discount_rate: float32 [2048], P('env'), may hold values from 3.0517579e-06 to 0.03
- trace_rate: float32 [2048], P('env'), may hold values from 3.0517579e-06 to 0.03
Outputs:
- norm_advantages: float32 [2048, 16384], P(('env', 'tm'))
- norm_returns: float32 [2048, 16384], P(('env', 'tm'))
The draws below stay inside these ranges and needn't reach their ends.
Inputs may be any that keep to these rules, and one draw needn't show every extreme that they name: `done_steps`: a repeated step in one environment's list is one termination.
All inputs are finite; a program needn't handle non-finite values.
Results may differ from the reference program's by a relative error of at most 0.0008.
Values sent between devices are 32-bit elements; how exact they have to be, the bound alone decides.
A program may use at most 128 MiB of HBM per device.

```python
import math
import jax
import jax.numpy as jnp
from jax import lax

EVENTS = 4
TSTEPS = 16384
ENVS = 2048
HORIZON = 8192


def touch_ends(result, rng, smallest, high):
    shape = result.shape
    spot = [jax.random.randint(jax.random.fold_in(rng, axis), (), 0, shape[axis]) for axis in range(len(shape))]
    result = result.at[tuple(spot)].set(smallest)
    longest = shape.index(max(shape))
    spot[longest] = (spot[longest] + 1) % shape[longest]
    return result.at[tuple(spot)].set(high)


def block_scale(own_key, dims, shards, least, largest):
    def one(axis_at, blocks):
        steps = jax.random.uniform(jax.random.fold_in(jax.random.fold_in(own_key, 6), axis_at), (blocks,), jnp.float32, least / len(shards), largest / len(shards))
        return jnp.repeat(jnp.exp(steps), dims[axis_at] // blocks).reshape((-1,) + (1,) * (len(dims) - axis_at - 1))

    loudness = one(*shards[0])
    for cut in shards[1:]:
        loudness = loudness * one(*cut)
    return loudness


def noise(key, shape, width, reach, cuts=(), kind=jnp.bfloat16):
    array = width * jax.random.normal(key, shape, jnp.float32)
    if cuts:
        array = array * block_scale(key, shape, cuts, -0.22, 0.18)
    return jnp.clip(array, -reach, reach).astype(kind)


def setup_inputs(seed: int = 0) -> dict:
    key_of = jax.random.split(jax.random.key(seed), 8)
    rewards = noise(key_of[0], (TSTEPS, ENVS), 0.02, 0.16, ((0, 8), (1, 4)), jnp.float32)
    values = noise(key_of[1], (TSTEPS, ENVS), 1.0, 6.0, ((0, 8), (1, 4)), jnp.float32)
    last_value = noise(key_of[2], (ENVS,), 1.0, 6.0, ((0, 4),), jnp.float32)
    done_steps = touch_ends(jax.random.randint(key_of[3], (ENVS, EVENTS), 0, TSTEPS), jax.random.fold_in(key_of[3], 1), 0, TSTEPS - 1).astype(jnp.int32)
    horizon_offset = touch_ends(jax.random.randint(key_of[4], (ENVS,), 0, HORIZON), jax.random.fold_in(key_of[4], 1), 0, HORIZON - 1).astype(jnp.int32)
    discount_rate = jnp.clip(jnp.exp(math.log(0.03) - 9.1932349 * jax.random.uniform(key_of[5], (ENVS,), jnp.float32) ** block_scale(key_of[5], (ENVS,), ((0, 4),), -0.2, 0.2)), 3.051757857974735e-06, 0.03)
    trace_rate = jnp.clip(jnp.exp(math.log(0.03) - 9.1932349 * jax.random.uniform(key_of[6], (ENVS,), jnp.float32) ** block_scale(key_of[6], (ENVS,), ((0, 4),), -0.2, 0.2)), 3.051757857974735e-06, 0.03)
    return dict(rewards=rewards, values=values, last_value=last_value, done_steps=done_steps, horizon_offset=horizon_offset, discount_rate=discount_rate, trace_rate=trace_rate)


def normalize(field):
    center = jnp.mean(field)
    spread = jnp.mean((field - center) * (field - center))
    return (field - center) / jnp.sqrt(spread + 1e-05)

def reference(rewards, values, last_value, done_steps, horizon_offset, discount_rate, trace_rate):
    moment_index = jnp.arange(TSTEPS, dtype=jnp.int32)
    discount = jnp.exp(-discount_rate)
    retention = discount * jnp.exp(-trace_rate)

    def backward(state, inputs):
        adv_next, value_next = state
        reward, value, moment = inputs
        finished = jnp.any(done_steps == moment, axis=1)
        truncated = (moment + horizon_offset) % HORIZON == HORIZON - 1
        living = 1.0 - finished.astype(rewards.dtype)
        carried = living * (1.0 - truncated.astype(rewards.dtype))
        td_error = reward + discount * living * value_next - value
        advantage = td_error + retention * carried * adv_next
        return ((advantage, value), advantage)
    start_state = (jnp.zeros_like(last_value), last_value)
    unused, advantages = lax.scan(backward, start_state, (rewards, values, moment_index), reverse=True)
    returns = advantages + values
    return (normalize(advantages).T, normalize(returns).T)
```

```python
import functools

import jax
import jax.numpy as jnp
from jax import lax
from jax.experimental import pallas as pl
from jax.experimental.pallas import tpu as pltpu
from jax.sharding import PartitionSpec as P

MESH = pl.DeviceIdType.MESH
CHUNKS = 4
SIDE = 128
PIECES = 4


def combine(parts):
    count = len(parts)
    means = [part[0:2] for part in parts]
    mean = functools.reduce(jnp.add, means) / count
    spread = [part[2:4] + (m - mean) * (m - mean) for part, m in zip(parts, means)]
    return mean, functools.reduce(jnp.add, spread) / count


def grid_of(n):
    side = 1 << ((n.bit_length() - 1) // 2)
    return n // side, side


def hops(n, i, j):
    side = grid_of(n)[1]
    return abs(i // side - j // side) + abs(i % side - j % side)


def plan(n, middle):
    lines, side = grid_of(n)
    mine = [i for i in range(n) if (i // side in (lines // 2 - 1, lines // 2)) == middle]
    reach = {d: max(hops(n, i, i ^ d) for i in mine) for d in range(1, n)}
    inside = [d for d in range(side, n // 2)]
    along = [d for d in range(1, side)]
    across = sorted(range(n // 2, n), key=lambda d: (reach[d], d % side) if middle else (-(d // side), d % side))
    return reach, inside, along, across


def exchange(
    n, m, horizon, samples,
    rewards, values, last_in, done_in, offset_in, rate_d_in, rate_t_in,
    out_a, out_v,
    last, done, offset, rate_d, rate_t,
    p_buf, v_buf, d_buf, vt, at, src, summary, st_one, env_stats, st_two, tm_stats,
    load_small, load_r, load_v, send_big, recv_v, recv_a, send_sum, recv_sum,
    send_env, recv_env, send_tm, recv_tm, gates,
):
    steps, envs = v_buf.shape
    rows = envs // n
    part = steps // CHUNKS
    me = lax.axis_index("tm")
    my_env = lax.axis_index("env")
    lines, side = grid_of(n)
    line, spot = me // side, lax.rem(me, side)
    middle = jnp.logical_or(line == lines // 2 - 1, line == lines // 2)
    peers = [jnp.bitwise_xor(me, d) for d in range(1, n)]
    mates = [lax.rem(my_env + d, m) for d in range(1, m)]

    neighbours = [
        (line > 0, me - side),
        (line < lines - 1, me + side),
        (spot > 0, me - 1),
        (spot < side - 1, me + 1),
    ]
    near = functools.reduce(jnp.add, [there.astype(jnp.int32) for there, unused in neighbours])

    def announce(sem):
        for there, peer in neighbours:
            @pl.when(there)
            def unused_tell():
                pl.semaphore_signal(sem, inc=1, device_id={"tm": peer}, device_id_type=MESH)

    barrier = pltpu.get_barrier_semaphore()
    for mate in mates:
        pl.semaphore_signal(barrier, inc=1, device_id={"env": mate}, device_id_type=MESH)
    announce(barrier)

    cuts = [(0, SIDE), (SIDE, part - SIDE)] + [(c * part, part) for c in range(1, CHUNKS)]
    loads_v = [
        pltpu.make_async_copy(
            values.at[pl.ds(t, size)], v_buf.at[pl.ds(t, size)], load_v.at[c]
        )
        for c, (t, size) in enumerate(cuts)
    ]
    loading_r = pltpu.make_async_copy(rewards, p_buf, load_r)
    loads_small = [
        pltpu.make_async_copy(source, target, load_small.at[i])
        for i, (source, target) in enumerate(
            ((done_in, done), (offset_in, offset), (rate_d_in, rate_d), (rate_t_in, rate_t), (last_in, last))
        )
    ]
    for load in loads_v + loads_small + [loading_r]:
        load.start()

    def send_part(which, source, target, sem, first, width, d):
        peer = peers[d - 1]
        pltpu.make_async_remote_copy(
            src_ref=source.at[
                pl.ds(pl.multiple_of(peer * rows, 8), rows), pl.ds(first, width)
            ],
            dst_ref=target.at[
                pl.ds(0, rows), pl.ds(pl.multiple_of(me * steps + first, SIDE), width)
            ],
            send_sem=send_big.at[which],
            recv_sem=sem,
            device_id={"tm": peer},
            device_id_type=MESH,
        ).start()

    def send_values(first, width, d):
        send_part(0, vt, out_v, recv_v.at[d - 1], first, width, d)

    def send_advantages(c, d):
        send_part(1, at, out_a, recv_a.at[(d - 1) * CHUNKS + c], c * part, part, d)

    def by_role(body):
        @pl.when(middle)
        def unused_middle():
            body(True, *plan(n, True))

        @pl.when(jnp.logical_not(middle))
        def unused_end():
            body(False, *plan(n, False))

    def turn_values(first, width):
        def body(b, unused):
            t = pl.multiple_of(first + b * SIDE, SIDE)
            for e in range(0, envs, SIDE):
                vt[pl.ds(e, SIDE), pl.ds(t, SIDE)] = v_buf[pl.ds(t, SIDE), pl.ds(e, SIDE)].T
            return unused

        lax.fori_loop(0, width // SIDE, body, 0)

    for load, (t, size) in zip(loads_v[:2], cuts[:2]):
        load.wait()
        turn_values(t, size)
    pl.semaphore_wait(barrier, near + m - 1)

    farthest = lines + side - 2
    for k in range(1, farthest + 1):
        if k > 1:
            pl.semaphore_wait(gates.at[k - 2], near)
        if k < farthest:
            announce(gates.at[k - 1])

        def first_sends(middle, reach, inside, along, across):
            for d in inside + across + along:
                if reach[d] == k:
                    for t, size in cuts[:2]:
                        send_values(t, size, d)

        by_role(first_sends)
        if k == 1:
            loads_v[2].wait()
            turn_values(part, part)

    def second_sends(middle, reach, inside, along, across):
        if middle:
            for d in across[: len(across) // 2]:
                send_values(part, part, d)

    by_role(second_sends)
    for c in range(2, CHUNKS):
        loads_v[c + 1].wait()
    loading_r.wait()
    for load in loads_small:
        load.wait()

    discount = jnp.exp(-rate_d[...])
    retention = discount * jnp.exp(-rate_t[...])
    first = me * steps
    wide = (8, envs)
    ends = [jnp.broadcast_to(done[j : j + 1, :] - first, wide) for j in range(done.shape[0])]
    resets = [
        jnp.broadcast_to(k * horizon - 1 - first - offset[...], wide)
        for k in (1, 2)
    ]
    disc = jnp.broadcast_to(discount, wide)
    keep = jnp.broadcast_to(retention, wide)
    row = lax.broadcasted_iota(jnp.int32, wide, 0)

    def tile(k, later, final):
        v_later, a_later, d_later = later
        at_rows = pl.ds(pl.multiple_of(k * 8, 8), 8)
        v = v_buf[at_rows, :]
        r = p_buf[at_rows, :]
        moment = row + k * 8
        finished = functools.reduce(jnp.logical_or, [moment == e for e in ends])
        stopped = functools.reduce(jnp.logical_or, [moment == e for e in resets], finished)
        reach = jnp.where(finished, 0.0, disc)
        decay = jnp.where(stopped, 0.0, keep)
        v_up = pltpu.roll(v, 7, 0)
        if final:
            src[3:4, :] = reach[7:8, :]
            src[4:5, :] = decay[7:8, :]
            td = r + jnp.where(row == 7, 0.0, reach * v_up) - v
            decay = jnp.where(row == 7, 1.0, decay)
        else:
            td = r + reach * jnp.where(row == 7, v_later, v_up) - v
        for s in (1, 2, 4):
            inside = row < 8 - s
            td_up = jnp.where(inside, pltpu.roll(td, 8 - s, 0), 0.0)
            decay_up = jnp.where(inside, pltpu.roll(decay, 8 - s, 0), 1.0)
            td = td + decay * td_up
            decay = decay * decay_up
        if not final:
            td = td + decay * a_later
            decay = decay * d_later
        p_buf[at_rows, :] = td
        d_buf[at_rows, :] = decay
        return (
            v_up,
            jnp.broadcast_to(td[0:1, :], wide),
            jnp.broadcast_to(decay[0:1, :], wide),
        )

    tiles = steps // 8
    state = tile(tiles - 1, (None, None, None), True)
    lax.fori_loop(0, tiles - 1, lambda i, s: tile(tiles - 2 - i, s, False), state)

    src[0:1, :] = p_buf[0:1, :]
    src[1:2, :] = d_buf[0:1, :]
    src[2:3, :] = v_buf[0:1, :]
    src[5:8, :] = jnp.zeros((3, envs), jnp.float32)
    summary[me] = src[...]
    for peer in peers:
        pltpu.make_async_remote_copy(
            src_ref=src, dst_ref=summary.at[me], send_sem=send_sum, recv_sem=recv_sum,
            device_id={"tm": peer}, device_id_type=MESH,
        ).start()
    turn_values(2 * part, steps - 2 * part)

    def other_sends(middle, reach, inside, along, across):
        early = across[: len(across) // 2] if middle else []
        for c in range(1, CHUNKS):
            for d in inside + along + across:
                if c > 1 or d not in early:
                    send_values(c * part, part, d)

    by_role(other_sends)

    def wait_all(source_like, sem):
        pltpu.make_async_copy(source_like, source_like, sem).wait()

    others = summary.at[pl.ds(0, n - 1)]
    wait_all(others, recv_sum)

    a_next = jnp.zeros((1, envs), jnp.float32)
    v_next = last[...]
    lift = jnp.zeros((1, envs), jnp.float32)
    for p in reversed(range(n)):
        block = summary[p]
        added = block[3:4] * v_next + block[4:5] * a_next
        lift = jnp.where(me == p, added, lift)
        a_next = block[0:1] + block[1:2] * added
        v_next = block[2:3]
    src_lift = [jnp.broadcast_to(lift[:, e : e + SIDE], (SIDE, SIDE)) for e in range(0, envs, SIDE)]

    def fold(x):
        return jnp.sum(x.reshape(SIDE // 8, 8, SIDE), axis=0)

    def finish(b, sums):
        sum_a, sum_v = sums
        t = pl.multiple_of(b * SIDE, SIDE)
        for i, e in enumerate(range(0, envs, SIDE)):
            here = (pl.ds(t, SIDE), pl.ds(e, SIDE))
            a = p_buf[here] + d_buf[here] * src_lift[i]
            at[pl.ds(e, SIDE), pl.ds(t, SIDE)] = a.T
            sum_a = sum_a + fold(a)
            sum_v = sum_v + fold(v_buf[here])
        return sum_a, sum_v

    zero = jnp.zeros((8, SIDE), jnp.float32)
    sum_a, sum_v = lax.fori_loop(0, steps // SIDE, finish, (zero, zero))
    total = lambda x: jnp.sum(jnp.sum(x, axis=1, keepdims=True), axis=0, keepdims=True)
    mean_a = total(sum_a) / samples
    mean_r = mean_a + total(sum_v) / samples
    span = 4 * SIDE
    mid_a = jnp.broadcast_to(mean_a, (8, span))
    mid_r = jnp.broadcast_to(mean_r, (8, span))

    def squares(i, sums):
        sq_a, sq_r = sums
        for t in range(0, steps, span):
            here = (pl.ds(pl.multiple_of(i * 8, 8), 8), pl.ds(t, span))
            a = at[here]
            dev_a = a - mid_a
            dev_r = (a + vt[here]) - mid_r
            sq_a = sq_a + dev_a * dev_a
            sq_r = sq_r + dev_r * dev_r
        return sq_a, sq_r

    zero = jnp.zeros((8, span), jnp.float32)
    sq_a, sq_r = lax.fori_loop(0, envs // 8, squares, (zero, zero))
    lane = (1, SIDE)
    st_one[0:1, :] = jnp.broadcast_to(mean_a, lane)
    st_one[1:2, :] = jnp.broadcast_to(mean_r, lane)
    st_one[2:3, :] = jnp.broadcast_to(total(sq_a) / samples, lane)
    st_one[3:4, :] = jnp.broadcast_to(total(sq_r) / samples, lane)
    st_one[4:8, :] = jnp.zeros((4, SIDE), jnp.float32)
    env_stats[my_env] = st_one[...]

    for mate in mates:
        pltpu.make_async_remote_copy(
            src_ref=st_one, dst_ref=env_stats.at[my_env], send_sem=send_env, recv_sem=recv_env,
            device_id={"env": mate}, device_id_type=MESH,
        ).start()
    def advantage_sends(chunks):
        def body(middle, reach, inside, along, across):
            for c in chunks:
                for d in inside + along + across:
                    send_advantages(c, d)

        by_role(body)

    advantage_sends((0, 1))
    wait_all(env_stats.at[pl.ds(0, m - 1)], recv_env)
    mean, var = combine([env_stats[q] for q in range(m)])
    st_two[0:2, :] = mean
    st_two[2:4, :] = var
    st_two[4:8, :] = jnp.zeros((4, SIDE), jnp.float32)
    tm_stats[me] = st_two[...]
    for peer in peers:
        pltpu.make_async_remote_copy(
            src_ref=st_two, dst_ref=tm_stats.at[me], send_sem=send_tm, recv_sem=recv_tm,
            device_id={"tm": peer}, device_id_type=MESH,
        ).start()
    advantage_sends(range(2, CHUNKS))

    wait_all(tm_stats.at[pl.ds(0, n - 1)], recv_tm)
    mean, var = combine([tm_stats[q] for q in range(n)])
    scale = lax.rsqrt(var + 1e-05)
    wide = (8, part)
    mid_a, mid_r, scale_a, scale_r = (
        jnp.broadcast_to(x[i : i + 1, 0:1], wide) for x in (mean, scale) for i in (0, 1)
    )

    def normalize(read_a, read_v, first):
        for r in range(0, rows, 8):
            here = (pl.ds(r, 8), pl.ds(first, part))
            a = read_a(r)
            v = read_v(r)
            out_a[here] = (a - mid_a) * scale_a
            out_v[here] = ((a + v) - mid_r) * scale_r

    def own(c, unused):
        def read(source):
            return lambda r: source[
                pl.ds(pl.multiple_of(me * rows + r, 8), 8),
                pl.ds(pl.multiple_of(c * part, SIDE), part),
            ]
        normalize(read(at), read(vt), pl.multiple_of(me * steps + c * part, SIDE))
        return unused

    lax.fori_loop(0, CHUNKS, own, 0)

    def arrived(place, c):
        first = pl.multiple_of(peers[place] * steps + c * part, SIDE)
        piece = out_a.at[:, pl.ds(0, part)]
        if c == 0:
            wait_all(out_v.at[:, pl.ds(0, steps)], recv_v.at[place])
        wait_all(piece, recv_a.at[place * CHUNKS + c])
        read = lambda source: lambda r: source[pl.ds(r, 8), pl.ds(first, part)]
        normalize(read(out_a), read(out_v), first)

    unused_reach, inside, along, across = plan(n, True)
    for c in range(CHUNKS):
        for d in inside + along + across[::-1]:
            arrived(d - 1, c)

    wait_all(others, send_sum)
    wait_all(env_stats.at[pl.ds(0, m - 1)], send_env)
    wait_all(tm_stats.at[pl.ds(0, n - 1)], send_tm)
    for which, source in enumerate((vt, at)):
        wait_all(source.at[pl.ds(0, (n - 1) * rows)], send_big.at[which])


def drain_kernel(a, v, out_a, out_v, sems):
    part = a.shape[0] // PIECES
    copies = [
        pltpu.make_async_copy(source.at[pl.ds(i * part, part)], target.at[pl.ds(i * part, part)], sems.at[k, i])
        for i in range(PIECES)
        for k, (source, target) in enumerate(((a, out_a), (v, out_v)))
    ]
    for copy in copies:
        copy.start()
    for copy in copies:
        copy.wait()


def drain(a, v):
    shape = jax.ShapeDtypeStruct(a.shape, a.dtype)
    local = pl.BlockSpec(memory_space=pltpu.VMEM)
    remote = pl.BlockSpec(memory_space=pltpu.HBM)
    return pl.pallas_call(
        drain_kernel,
        out_shape=(shape, shape),
        in_specs=(local, local),
        out_specs=(remote, remote),
        scratch_shapes=[pltpu.SemaphoreType.DMA((2, PIECES))],
        compiler_params=pltpu.CompilerParams(vmem_limit_bytes=1024 * 1024),
    )(a, v)


def shards(rewards, values, last_value, done_steps, horizon_offset, discount_rate, trace_rate):
    steps, envs = rewards.shape
    n, m = lax.axis_size("tm"), lax.axis_size("env")
    rows = envs // n
    horizon = steps * n // 2
    whole = pltpu.VMEM((rows, steps * n), jnp.float32)
    kernel = functools.partial(exchange, n, m, horizon, float(steps * envs))
    remote = pl.BlockSpec(memory_space=pltpu.HBM)
    local = pl.BlockSpec(memory_space=pltpu.VMEM)
    f32 = jnp.float32
    dma = pltpu.SemaphoreType.DMA
    a, v = pl.pallas_call(
        kernel,
        out_shape=(whole, whole),
        in_specs=[remote] * 7,
        out_specs=(local, local),
        scratch_shapes=[
            pltpu.VMEM((1, envs), f32),
            pltpu.VMEM(done_steps.shape[::-1], jnp.int32),
            pltpu.VMEM((1, envs), jnp.int32),
            pltpu.VMEM((1, envs), f32),
            pltpu.VMEM((1, envs), f32),
            pltpu.VMEM((steps, envs), f32),
            pltpu.VMEM((steps, envs), f32),
            pltpu.VMEM((steps, envs), f32),
            pltpu.VMEM((envs, steps), f32),
            pltpu.VMEM((envs, steps), f32),
            pltpu.VMEM((8, envs), f32),
            pltpu.VMEM((n, 8, envs), f32),
            pltpu.VMEM((8, SIDE), f32),
            pltpu.VMEM((m, 8, SIDE), f32),
            pltpu.VMEM((8, SIDE), f32),
            pltpu.VMEM((n, 8, SIDE), f32),
            dma((5,)), dma, dma((CHUNKS + 1,)), dma((2,)), dma((n - 1,)), dma(((n - 1) * CHUNKS,)), dma, dma,
            dma, dma, dma, dma, pltpu.SemaphoreType.REGULAR((n,)),
        ],
        compiler_params=pltpu.CompilerParams(
            collective_id=0, has_side_effects=True, vmem_limit_bytes=55 * 1024 * 1024
        ),
    )(
        rewards,
        values,
        last_value[None, :],
        done_steps.T,
        horizon_offset[None, :],
        discount_rate[None, :],
        trace_rate[None, :],
    )
    return drain(a, v)


def solution(mesh):
    in_specs = (
        P("tm", "env"),
        P("tm", "env"),
        P("env"),
        P("env", None),
        P("env"),
        P("env"),
        P("env"),
    )
    out_specs = (P(("env", "tm"), None), P(("env", "tm"), None))
    return jax.shard_map(shards, mesh=mesh, in_specs=in_specs, out_specs=out_specs, check_vma=False)
```

```python
import functools

import jax
import jax.numpy as jnp
from jax import lax
from jax.experimental import pallas as pl
from jax.experimental.pallas import tpu as pltpu
from jax.sharding import PartitionSpec as P

MESH = pl.DeviceIdType.MESH
CHUNKS = 4
SIDE = 128
PIECES = 4
HELD = 1
HELD_TILL = 3


def combine(parts):
    count = len(parts)
    means = [part[0:2] for part in parts]
    mean = functools.reduce(jnp.add, means) / count
    spread = [part[2:4] + (m - mean) * (m - mean) for part, m in zip(parts, means)]
    return mean, functools.reduce(jnp.add, spread) / count


def grid_of(n):
    side = 1 << ((n.bit_length() - 1) // 2)
    return n // side, side


def hops(n, i, j):
    side = grid_of(n)[1]
    return abs(i // side - j // side) + abs(i % side - j % side)


def plan(n, middle):
    lines, side = grid_of(n)
    mine = [i for i in range(n) if (i // side in (lines // 2 - 1, lines // 2)) == middle]
    reach = {d: max(hops(n, i, i ^ d) for i in mine) for d in range(1, n)}
    inside = [d for d in range(side, n // 2)]
    along = [d for d in range(1, side)]
    across = sorted(range(n // 2, n), key=lambda d: (reach[d], d % side) if middle else (-(d // side), d % side))
    return reach, inside, along, across


def exchange(
    n, m, horizon, samples,
    rewards, values, last_in, done_in, offset_in, rate_d_in, rate_t_in,
    out_a, out_v,
    last, done, offset, rate_d, rate_t,
    p_buf, v_buf, d_buf, vt, at, src, summary, st_one, env_stats, st_two, tm_stats,
    load_small, load_r, load_v, send_big, recv_v, recv_a, send_sum, recv_sum,
    send_env, recv_env, send_tm, recv_tm, gates,
):
    steps, envs = v_buf.shape
    rows = envs // n
    part = steps // CHUNKS
    me = lax.axis_index("tm")
    my_env = lax.axis_index("env")
    lines, side = grid_of(n)
    line, spot = me // side, lax.rem(me, side)
    middle = jnp.logical_or(line == lines // 2 - 1, line == lines // 2)
    peers = [jnp.bitwise_xor(me, d) for d in range(1, n)]
    mates = [lax.rem(my_env + d, m) for d in range(1, m)]

    neighbours = [
        (line > 0, me - side),
        (line < lines - 1, me + side),
        (spot > 0, me - 1),
        (spot < side - 1, me + 1),
    ]
    near = functools.reduce(jnp.add, [there.astype(jnp.int32) for there, unused in neighbours])

    def announce(sem):
        for there, peer in neighbours:
            @pl.when(there)
            def unused_tell():
                pl.semaphore_signal(sem, inc=1, device_id={"tm": peer}, device_id_type=MESH)

    barrier = pltpu.get_barrier_semaphore()
    for mate in mates:
        pl.semaphore_signal(barrier, inc=1, device_id={"env": mate}, device_id_type=MESH)
    announce(barrier)

    cuts = [(0, SIDE), (SIDE, part - SIDE)] + [(c * part, part) for c in range(1, CHUNKS)]
    loads_v = [
        pltpu.make_async_copy(
            values.at[pl.ds(t, size)], v_buf.at[pl.ds(t, size)], load_v.at[c]
        )
        for c, (t, size) in enumerate(cuts)
    ]
    loading_r = pltpu.make_async_copy(rewards, p_buf, load_r)
    loads_small = [
        pltpu.make_async_copy(source, target, load_small.at[i])
        for i, (source, target) in enumerate(
            ((done_in, done), (offset_in, offset), (rate_d_in, rate_d), (rate_t_in, rate_t), (last_in, last))
        )
    ]
    for load in loads_v + loads_small + [loading_r]:
        load.start()

    def send_part(which, source, target, sem, first, width, d):
        peer = peers[d - 1]
        pltpu.make_async_remote_copy(
            src_ref=source.at[
                pl.ds(pl.multiple_of(peer * rows, 8), rows), pl.ds(first, width)
            ],
            dst_ref=target.at[
                pl.ds(0, rows), pl.ds(pl.multiple_of(me * steps + first, SIDE), width)
            ],
            send_sem=send_big.at[which],
            recv_sem=sem,
            device_id={"tm": peer},
            device_id_type=MESH,
        ).start()

    def send_values(first, width, d):
        send_part(0, vt, out_v, recv_v.at[d - 1], first, width, d)

    def send_advantages(c, d):
        send_part(1, at, out_a, recv_a.at[(d - 1) * CHUNKS + c], c * part, part, d)

    def by_role(body):
        @pl.when(middle)
        def unused_middle():
            body(True, *plan(n, True))

        @pl.when(jnp.logical_not(middle))
        def unused_end():
            body(False, *plan(n, False))

    def turn_values(first, width):
        def body(b, unused):
            t = pl.multiple_of(first + b * SIDE, SIDE)
            for e in range(0, envs, SIDE):
                vt[pl.ds(e, SIDE), pl.ds(t, SIDE)] = v_buf[pl.ds(t, SIDE), pl.ds(e, SIDE)].T
            return unused

        lax.fori_loop(0, width // SIDE, body, 0)

    for load, (t, size) in zip(loads_v[:2], cuts[:2]):
        load.wait()
        turn_values(t, size)
    pl.semaphore_wait(barrier, near + m - 1)

    farthest = lines + side - 2
    for k in range(1, farthest + 1):
        if k > 1:
            pl.semaphore_wait(gates.at[k - 2], near)
        if k < farthest:
            announce(gates.at[k - 1])

        def first_sends(middle, reach, inside, along, across):
            for d in inside + across + along:
                if reach[d] == k:
                    for t, size in cuts[:2]:
                        send_values(t, size, d)

        by_role(first_sends)
        if k == 1:
            loads_v[2].wait()
            turn_values(part, part)

    def second_sends(middle, reach, inside, along, across):
        if middle:
            for d in across[: len(across) // 2]:
                send_values(part, part, d)

    by_role(second_sends)
    for c in range(2, CHUNKS):
        loads_v[c + 1].wait()
    loading_r.wait()
    for load in loads_small:
        load.wait()

    discount = jnp.exp(-rate_d[...])
    retention = discount * jnp.exp(-rate_t[...])
    first = me * steps
    wide = (8, envs)
    ends = [jnp.broadcast_to(done[j : j + 1, :] - first, wide) for j in range(done.shape[0])]
    resets = [
        jnp.broadcast_to(k * horizon - 1 - first - offset[...], wide)
        for k in (1, 2)
    ]
    disc = jnp.broadcast_to(discount, wide)
    keep = jnp.broadcast_to(retention, wide)
    row = lax.broadcasted_iota(jnp.int32, wide, 0)

    def tile(k, later, final):
        v_later, a_later, d_later = later
        at_rows = pl.ds(pl.multiple_of(k * 8, 8), 8)
        v = v_buf[at_rows, :]
        r = p_buf[at_rows, :]
        moment = row + k * 8
        finished = functools.reduce(jnp.logical_or, [moment == e for e in ends])
        stopped = functools.reduce(jnp.logical_or, [moment == e for e in resets], finished)
        reach = jnp.where(finished, 0.0, disc)
        decay = jnp.where(stopped, 0.0, keep)
        v_up = pltpu.roll(v, 7, 0)
        if final:
            src[3:4, :] = reach[7:8, :]
            src[4:5, :] = decay[7:8, :]
            td = r + jnp.where(row == 7, 0.0, reach * v_up) - v
            decay = jnp.where(row == 7, 1.0, decay)
        else:
            td = r + reach * jnp.where(row == 7, v_later, v_up) - v
        for s in (1, 2, 4):
            inside = row < 8 - s
            td_up = jnp.where(inside, pltpu.roll(td, 8 - s, 0), 0.0)
            decay_up = jnp.where(inside, pltpu.roll(decay, 8 - s, 0), 1.0)
            td = td + decay * td_up
            decay = decay * decay_up
        if not final:
            td = td + decay * a_later
            decay = decay * d_later
        p_buf[at_rows, :] = td
        d_buf[at_rows, :] = decay
        return (
            v_up,
            jnp.broadcast_to(td[0:1, :], wide),
            jnp.broadcast_to(decay[0:1, :], wide),
        )

    tiles = steps // 8
    state = tile(tiles - 1, (None, None, None), True)
    lax.fori_loop(0, tiles - 1, lambda i, s: tile(tiles - 2 - i, s, False), state)

    src[0:1, :] = p_buf[0:1, :]
    src[1:2, :] = d_buf[0:1, :]
    src[2:3, :] = v_buf[0:1, :]
    src[5:8, :] = jnp.zeros((3, envs), jnp.float32)
    summary[me] = src[...]
    for peer in peers:
        pltpu.make_async_remote_copy(
            src_ref=src, dst_ref=summary.at[me], send_sem=send_sum, recv_sem=recv_sum,
            device_id={"tm": peer}, device_id_type=MESH,
        ).start()
    turn_values(2 * part, steps - 2 * part)

    def other_sends(middle, reach, inside, along, across):
        early = across[: len(across) // 2] if middle else []
        for c in range(1, CHUNKS):
            for d in inside + along + across:
                if c > 1 or d not in early:
                    send_values(c * part, part, d)

    by_role(other_sends)

    def wait_all(source_like, sem):
        pltpu.make_async_copy(source_like, source_like, sem).wait()

    others = summary.at[pl.ds(0, n - 1)]
    wait_all(others, recv_sum)

    a_next = jnp.zeros((1, envs), jnp.float32)
    v_next = last[...]
    lift = jnp.zeros((1, envs), jnp.float32)
    for p in reversed(range(n)):
        block = summary[p]
        added = block[3:4] * v_next + block[4:5] * a_next
        lift = jnp.where(me == p, added, lift)
        a_next = block[0:1] + block[1:2] * added
        v_next = block[2:3]
    src_lift = [jnp.broadcast_to(lift[:, e : e + SIDE], (SIDE, SIDE)) for e in range(0, envs, SIDE)]

    def fold(x):
        return jnp.sum(x.reshape(SIDE // 8, 8, SIDE), axis=0)

    def finish(b, sums):
        sum_a, sum_v = sums
        t = pl.multiple_of(b * SIDE, SIDE)
        for i, e in enumerate(range(0, envs, SIDE)):
            here = (pl.ds(t, SIDE), pl.ds(e, SIDE))
            a = p_buf[here] + d_buf[here] * src_lift[i]
            at[pl.ds(e, SIDE), pl.ds(t, SIDE)] = a.T
            sum_a = sum_a + fold(a)
            sum_v = sum_v + fold(v_buf[here])
        return sum_a, sum_v

    zero = jnp.zeros((8, SIDE), jnp.float32)
    sum_a, sum_v = lax.fori_loop(0, steps // SIDE, finish, (zero, zero))
    total = lambda x: jnp.sum(jnp.sum(x, axis=1, keepdims=True), axis=0, keepdims=True)
    mean_a = total(sum_a) / samples
    mean_r = mean_a + total(sum_v) / samples
    span = 4 * SIDE
    mid_a = jnp.broadcast_to(mean_a, (8, span))
    mid_r = jnp.broadcast_to(mean_r, (8, span))

    def squares(i, sums):
        sq_a, sq_r = sums
        for t in range(0, steps, span):
            here = (pl.ds(pl.multiple_of(i * 8, 8), 8), pl.ds(t, span))
            a = at[here]
            dev_a = a - mid_a
            dev_r = (a + vt[here]) - mid_r
            sq_a = sq_a + dev_a * dev_a
            sq_r = sq_r + dev_r * dev_r
        return sq_a, sq_r

    zero = jnp.zeros((8, span), jnp.float32)
    sq_a, sq_r = lax.fori_loop(0, envs // 8, squares, (zero, zero))
    lane = (1, SIDE)
    st_one[0:1, :] = jnp.broadcast_to(mean_a, lane)
    st_one[1:2, :] = jnp.broadcast_to(mean_r, lane)
    st_one[2:3, :] = jnp.broadcast_to(total(sq_a) / samples, lane)
    st_one[3:4, :] = jnp.broadcast_to(total(sq_r) / samples, lane)
    st_one[4:8, :] = jnp.zeros((4, SIDE), jnp.float32)
    env_stats[my_env] = st_one[...]

    for mate in mates:
        pltpu.make_async_remote_copy(
            src_ref=st_one, dst_ref=env_stats.at[my_env], send_sem=send_env, recv_sem=recv_env,
            device_id={"env": mate}, device_id_type=MESH,
        ).start()
    def advantage_sends(chunks):
        def body(middle, reach, inside, along, across):
            for c in chunks:
                for d in inside + along + across:
                    if not (middle and d in across and c >= CHUNKS - HELD):
                        send_advantages(c, d)

        by_role(body)

    advantage_sends((0, 1))
    wait_all(env_stats.at[pl.ds(0, m - 1)], recv_env)
    mean, var = combine([env_stats[q] for q in range(m)])
    st_two[0:2, :] = mean
    st_two[2:4, :] = var
    st_two[4:8, :] = jnp.zeros((4, SIDE), jnp.float32)
    tm_stats[me] = st_two[...]
    for peer in peers:
        pltpu.make_async_remote_copy(
            src_ref=st_two, dst_ref=tm_stats.at[me], send_sem=send_tm, recv_sem=recv_tm,
            device_id={"tm": peer}, device_id_type=MESH,
        ).start()
    advantage_sends(range(2, CHUNKS))

    wait_all(tm_stats.at[pl.ds(0, n - 1)], recv_tm)
    mean, var = combine([tm_stats[q] for q in range(n)])
    scale = lax.rsqrt(var + 1e-05)
    wide = (8, part)
    mid_a, mid_r, scale_a, scale_r = (
        jnp.broadcast_to(x[i : i + 1, 0:1], wide) for x in (mean, scale) for i in (0, 1)
    )

    def normalize(read_a, read_v, first):
        for r in range(0, rows, 8):
            here = (pl.ds(r, 8), pl.ds(first, part))
            a = read_a(r)
            v = read_v(r)
            out_a[here] = (a - mid_a) * scale_a
            out_v[here] = ((a + v) - mid_r) * scale_r

    def own(c, unused):
        def read(source):
            return lambda r: source[
                pl.ds(pl.multiple_of(me * rows + r, 8), 8),
                pl.ds(pl.multiple_of(c * part, SIDE), part),
            ]
        normalize(read(at), read(vt), pl.multiple_of(me * steps + c * part, SIDE))
        return unused

    lax.fori_loop(0, CHUNKS, own, 0)

    def landed(place, c):
        if c == 0:
            wait_all(out_v.at[:, pl.ds(0, steps)], recv_v.at[place])
        wait_all(out_a.at[:, pl.ds(0, part)], recv_a.at[place * CHUNKS + c])

    def arrived(place, c, waited):
        first = pl.multiple_of(peers[place] * steps + c * part, SIDE)
        if not waited:
            landed(place, c)
        read = lambda source: lambda r: source[pl.ds(r, 8), pl.ds(first, part)]
        normalize(read(out_a), read(out_v), first)

    unused_reach, inside, along, across = plan(n, True)
    far = [d for d in across if lines // 2 <= d // side < lines - 1]
    for c in range(HELD_TILL):
        for d in far:
            landed(d - 1, c)

    @pl.when(middle)
    def unused_held():
        for c in range(CHUNKS - HELD, CHUNKS):
            for d in across[::-1]:
                send_advantages(c, d)

    for c in range(CHUNKS):
        for d in inside + along + across[::-1]:
            arrived(d - 1, c, d in far and c < HELD_TILL)

    wait_all(others, send_sum)
    wait_all(env_stats.at[pl.ds(0, m - 1)], send_env)
    wait_all(tm_stats.at[pl.ds(0, n - 1)], send_tm)
    for which, source in enumerate((vt, at)):
        wait_all(source.at[pl.ds(0, (n - 1) * rows)], send_big.at[which])


def drain_kernel(a, v, out_a, out_v, sems):
    part = a.shape[0] // PIECES
    copies = [
        pltpu.make_async_copy(source.at[pl.ds(i * part, part)], target.at[pl.ds(i * part, part)], sems.at[k, i])
        for i in range(PIECES)
        for k, (source, target) in enumerate(((a, out_a), (v, out_v)))
    ]
    for copy in copies:
        copy.start()
    for copy in copies:
        copy.wait()


def drain(a, v):
    shape = jax.ShapeDtypeStruct(a.shape, a.dtype)
    local = pl.BlockSpec(memory_space=pltpu.VMEM)
    remote = pl.BlockSpec(memory_space=pltpu.HBM)
    return pl.pallas_call(
        drain_kernel,
        out_shape=(shape, shape),
        in_specs=(local, local),
        out_specs=(remote, remote),
        scratch_shapes=[pltpu.SemaphoreType.DMA((2, PIECES))],
        compiler_params=pltpu.CompilerParams(vmem_limit_bytes=1024 * 1024),
    )(a, v)


def shards(rewards, values, last_value, done_steps, horizon_offset, discount_rate, trace_rate):
    steps, envs = rewards.shape
    n, m = lax.axis_size("tm"), lax.axis_size("env")
    rows = envs // n
    horizon = steps * n // 2
    whole = pltpu.VMEM((rows, steps * n), jnp.float32)
    kernel = functools.partial(exchange, n, m, horizon, float(steps * envs))
    remote = pl.BlockSpec(memory_space=pltpu.HBM)
    local = pl.BlockSpec(memory_space=pltpu.VMEM)
    f32 = jnp.float32
    dma = pltpu.SemaphoreType.DMA
    a, v = pl.pallas_call(
        kernel,
        out_shape=(whole, whole),
        in_specs=[remote] * 7,
        out_specs=(local, local),
        scratch_shapes=[
            pltpu.VMEM((1, envs), f32),
            pltpu.VMEM(done_steps.shape[::-1], jnp.int32),
            pltpu.VMEM((1, envs), jnp.int32),
            pltpu.VMEM((1, envs), f32),
            pltpu.VMEM((1, envs), f32),
            pltpu.VMEM((steps, envs), f32),
            pltpu.VMEM((steps, envs), f32),
            pltpu.VMEM((steps, envs), f32),
            pltpu.VMEM((envs, steps), f32),
            pltpu.VMEM((envs, steps), f32),
            pltpu.VMEM((8, envs), f32),
            pltpu.VMEM((n, 8, envs), f32),
            pltpu.VMEM((8, SIDE), f32),
            pltpu.VMEM((m, 8, SIDE), f32),
            pltpu.VMEM((8, SIDE), f32),
            pltpu.VMEM((n, 8, SIDE), f32),
            dma((5,)), dma, dma((CHUNKS + 1,)), dma((2,)), dma((n - 1,)), dma(((n - 1) * CHUNKS,)), dma, dma,
            dma, dma, dma, dma, pltpu.SemaphoreType.REGULAR((n,)),
        ],
        compiler_params=pltpu.CompilerParams(
            collective_id=0, has_side_effects=True, vmem_limit_bytes=55 * 1024 * 1024
        ),
    )(
        rewards,
        values,
        last_value[None, :],
        done_steps.T,
        horizon_offset[None, :],
        discount_rate[None, :],
        trace_rate[None, :],
    )
    return drain(a, v)


def solution(mesh):
    in_specs = (
        P("tm", "env"),
        P("tm", "env"),
        P("env"),
        P("env", None),
        P("env"),
        P("env"),
        P("env"),
    )
    out_specs = (P(("env", "tm"), None), P(("env", "tm"), None))
    return jax.shard_map(shards, mesh=mesh, in_specs=in_specs, out_specs=out_specs, check_vma=False)
```

```python
import functools

import jax
import jax.numpy as jnp
from jax import lax
from jax.experimental import pallas as pl
from jax.experimental.pallas import tpu as pltpu
from jax.sharding import PartitionSpec as P

MESH = pl.DeviceIdType.MESH
CHUNKS = 4
SIDE = 128
PIECES = 4
HELD = 1
HELD_TILL = 2
EARLY = 2


def combine(parts):
    count = len(parts)
    means = [part[0:1] for part in parts]
    mean = functools.reduce(jnp.add, means) / count
    spread = [part[1:2] + (m - mean) * (m - mean) for part, m in zip(parts, means)]
    return mean, functools.reduce(jnp.add, spread) / count


def grid_of(n):
    side = 1 << ((n.bit_length() - 1) // 2)
    return n // side, side


def hops(n, i, j):
    side = grid_of(n)[1]
    return abs(i // side - j // side) + abs(i % side - j % side)


def plan(n, middle):
    lines, side = grid_of(n)
    mine = [i for i in range(n) if (i // side in (lines // 2 - 1, lines // 2)) == middle]
    reach = {d: max(hops(n, i, i ^ d) for i in mine) for d in range(1, n)}
    inside = [d for d in range(side, n // 2)]
    along = [d for d in range(1, side)]
    across = sorted(range(n // 2, n), key=lambda d: (reach[d], d % side) if middle else (-(d // side), d % side))
    return reach, inside, along, across


def exchange(
    n, m, horizon, samples,
    rewards, values, last_in, done_in, offset_in, rate_d_in, rate_t_in,
    out_a, out_v,
    last, done, offset, rate_d, rate_t,
    p_buf, v_buf, d_buf, vt, at, src, summary, border, entry, st_one, env_stats, st_two, tm_stats,
    load_small, load_r, load_v, send_big, recv_v, recv_a, send_sum, recv_sum, send_border, recv_border,
    send_env, recv_env, send_tm, recv_tm, gates,
):
    steps, envs = v_buf.shape
    rows = envs // n
    part = steps // CHUNKS
    me = lax.axis_index("tm")
    my_env = lax.axis_index("env")
    lines, side = grid_of(n)
    line, spot = me // side, lax.rem(me, side)
    middle = jnp.logical_or(line == lines // 2 - 1, line == lines // 2)
    peers = [jnp.bitwise_xor(me, d) for d in range(1, n)]
    mates = [lax.rem(my_env + d, m) for d in range(1, m)]

    neighbours = [
        (line > 0, me - side),
        (line < lines - 1, me + side),
        (spot > 0, me - 1),
        (spot < side - 1, me + 1),
    ]
    near = functools.reduce(jnp.add, [there.astype(jnp.int32) for there, unused in neighbours])

    def announce(sem):
        for there, peer in neighbours:
            @pl.when(there)
            def unused_tell():
                pl.semaphore_signal(sem, inc=1, device_id={"tm": peer}, device_id_type=MESH)

    barrier = pltpu.get_barrier_semaphore()
    for mate in mates:
        pl.semaphore_signal(barrier, inc=1, device_id={"env": mate}, device_id_type=MESH)
    announce(barrier)

    cuts = [(0, SIDE), (SIDE, part - SIDE)] + [(c * part, part) for c in range(1, CHUNKS)]
    loads_v = [
        pltpu.make_async_copy(
            values.at[pl.ds(t, size)], v_buf.at[pl.ds(t, size)], load_v.at[c]
        )
        for c, (t, size) in enumerate(cuts)
    ]
    loading_r = pltpu.make_async_copy(rewards, p_buf, load_r)
    loads_small = [
        pltpu.make_async_copy(source, target, load_small.at[i])
        for i, (source, target) in enumerate(
            ((done_in, done), (offset_in, offset), (rate_d_in, rate_d), (rate_t_in, rate_t), (last_in, last))
        )
    ]
    for load in loads_v + loads_small + [loading_r]:
        load.start()

    def send_part(which, source, target, sem, first, width, d):
        peer = peers[d - 1]
        pltpu.make_async_remote_copy(
            src_ref=source.at[
                pl.ds(pl.multiple_of(peer * rows, 8), rows), pl.ds(first, width)
            ],
            dst_ref=target.at[
                pl.ds(0, rows), pl.ds(pl.multiple_of(me * steps + first, SIDE), width)
            ],
            send_sem=send_big.at[which],
            recv_sem=sem,
            device_id={"tm": peer},
            device_id_type=MESH,
        ).start()

    def send_values(first, width, d):
        send_part(0, vt, out_v, recv_v.at[d - 1], first, width, d)

    def send_advantages(c, d):
        send_part(1, at, out_a, recv_a.at[(d - 1) * CHUNKS + c], c * part, part, d)

    def by_role(body):
        @pl.when(middle)
        def unused_middle():
            body(True, *plan(n, True))

        @pl.when(jnp.logical_not(middle))
        def unused_end():
            body(False, *plan(n, False))

    def turn_values(first, width):
        def body(b, unused):
            t = pl.multiple_of(first + b * SIDE, SIDE)
            for e in range(0, envs, SIDE):
                vt[pl.ds(e, SIDE), pl.ds(t, SIDE)] = v_buf[pl.ds(t, SIDE), pl.ds(e, SIDE)].T
            return unused

        lax.fori_loop(0, width // SIDE, body, 0)

    for load, (t, size) in zip(loads_v[:2], cuts[:2]):
        load.wait()
        turn_values(t, size)
    pl.semaphore_wait(barrier, near + m - 1)

    farthest = lines + side - 2
    for k in range(1, farthest + 1):
        if k > 1:
            pl.semaphore_wait(gates.at[k - 2], near)
        if k < farthest:
            announce(gates.at[k - 1])

        def first_sends(middle, reach, inside, along, across):
            for d in inside + (across if middle else []) + along:
                if reach[d] == k:
                    for t, size in cuts[:2]:
                        send_values(t, size, d)

        by_role(first_sends)
        if k == 1:
            loads_v[2].wait()
            turn_values(part, part)

    def second_sends(middle, reach, inside, along, across):
        for d in across[:EARLY] if middle else inside + along:
            send_values(part, part, d)

    by_role(second_sends)
    for c in range(2, CHUNKS):
        loads_v[c + 1].wait()
    loading_r.wait()
    for load in loads_small:
        load.wait()

    discount = jnp.exp(-rate_d[...])
    retention = discount * jnp.exp(-rate_t[...])
    first = me * steps
    wide = (8, envs)
    ends = [jnp.broadcast_to(done[j : j + 1, :] - first, wide) for j in range(done.shape[0])]
    resets = [
        jnp.broadcast_to(k * horizon - 1 - first - offset[...], wide)
        for k in (1, 2)
    ]
    disc = jnp.broadcast_to(discount, wide)
    keep = jnp.broadcast_to(retention, wide)
    row = lax.broadcasted_iota(jnp.int32, wide, 0)

    def tile(k, later, final):
        v_later, a_later, d_later = later
        at_rows = pl.ds(pl.multiple_of(k * 8, 8), 8)
        v = v_buf[at_rows, :]
        r = p_buf[at_rows, :]
        moment = row + k * 8
        finished = functools.reduce(jnp.logical_or, [moment == e for e in ends])
        stopped = functools.reduce(jnp.logical_or, [moment == e for e in resets], finished)
        reach = jnp.where(finished, 0.0, disc)
        decay = jnp.where(stopped, 0.0, keep)
        v_up = pltpu.roll(v, 7, 0)
        if final:
            src[3:4, :] = reach[7:8, :]
            src[4:5, :] = decay[7:8, :]
            td = r + jnp.where(row == 7, 0.0, reach * v_up) - v
            decay = jnp.where(row == 7, 1.0, decay)
        else:
            td = r + reach * jnp.where(row == 7, v_later, v_up) - v
        for s in (1, 2, 4):
            inside = row < 8 - s
            td_up = jnp.where(inside, pltpu.roll(td, 8 - s, 0), 0.0)
            decay_up = jnp.where(inside, pltpu.roll(decay, 8 - s, 0), 1.0)
            td = td + decay * td_up
            decay = decay * decay_up
        if not final:
            td = td + decay * a_later
            decay = decay * d_later
        p_buf[at_rows, :] = td
        d_buf[at_rows, :] = decay
        return (
            v_up,
            jnp.broadcast_to(td[0:1, :], wide),
            jnp.broadcast_to(decay[0:1, :], wide),
        )

    tiles = steps // 8
    state = tile(tiles - 1, (None, None, None), True)
    lax.fori_loop(0, tiles - 1, lambda i, s: tile(tiles - 2 - i, s, False), state)

    src[0:1, :] = p_buf[0:1, :]
    src[1:2, :] = d_buf[0:1, :]
    src[2:3, :] = v_buf[0:1, :]
    src[5:8, :] = jnp.zeros((3, envs), jnp.float32)
    half = n // 2
    place = lax.rem(me, half)
    later = me >= half
    summary[place] = src[...]
    for d in range(1, half):
        pltpu.make_async_remote_copy(
            src_ref=src, dst_ref=summary.at[place], send_sem=send_sum, recv_sem=recv_sum,
            device_id={"tm": peers[d - 1]}, device_id_type=MESH,
        ).start()

    def other_sends(middle, reach, inside, along, across):
        for c in range(CHUNKS):
            near_by = inside + along
            if c < (1 if middle else 2):
                near_by = []
            far_side = across
            if middle and c == 0:
                far_side = []
            if middle and c == 1:
                far_side = across[EARLY:]
            for d in near_by + far_side:
                if c == 0:
                    for t, size in cuts[:2]:
                        send_values(t, size, d)
                else:
                    send_values(c * part, part, d)

    def wait_all(source_like, sem):
        pltpu.make_async_copy(source_like, source_like, sem).wait()

    turn_values(2 * part, steps - 2 * part)

    @pl.when(jnp.logical_not(later))
    def unused_send_early():
        by_role(other_sends)

    others = summary.at[pl.ds(0, half - 1)]
    wait_all(others, recv_sum)

    crossing = pltpu.make_async_remote_copy(
        src_ref=border, dst_ref=entry, send_sem=send_border, recv_sem=recv_border,
        device_id={"tm": peers[half - 1]}, device_id_type=MESH,
    )

    @pl.when(later)
    def unused_last():
        entry[0:1, :] = jnp.zeros((1, envs), jnp.float32)
        entry[1:2, :] = last[...]

    @pl.when(jnp.logical_not(later))
    def unused_entry():
        crossing.wait_recv()

    a_next = entry[0:1, :]
    v_next = entry[1:2, :]
    lift = jnp.zeros((1, envs), jnp.float32)
    for p in reversed(range(half)):
        block = summary[p]
        added = block[3:4] * v_next + block[4:5] * a_next
        lift = jnp.where(place == p, added, lift)
        a_next = block[0:1] + block[1:2] * added
        v_next = block[2:3]
    border[0:1, :] = a_next
    border[1:2, :] = v_next

    @pl.when(later)
    def unused_cross():
        crossing.start()
        by_role(other_sends)

    src_lift = [jnp.broadcast_to(lift[:, e : e + SIDE], (SIDE, SIDE)) for e in range(0, envs, SIDE)]

    def fold(x):
        return jnp.sum(x.reshape(SIDE // 8, 8, SIDE), axis=0)

    def finish(b, sums):
        sum_a, sum_v = sums
        t = pl.multiple_of(b * SIDE, SIDE)
        for i, e in enumerate(range(0, envs, SIDE)):
            here = (pl.ds(t, SIDE), pl.ds(e, SIDE))
            a = p_buf[here] + d_buf[here] * src_lift[i]
            at[pl.ds(e, SIDE), pl.ds(t, SIDE)] = a.T
            sum_a = sum_a + fold(a)
            sum_v = sum_v + fold(v_buf[here])
        return sum_a, sum_v

    zero = jnp.zeros((8, SIDE), jnp.float32)
    sum_a, sum_v = lax.fori_loop(0, steps // SIDE, finish, (zero, zero))
    total = lambda x: jnp.sum(jnp.sum(x, axis=1, keepdims=True), axis=0, keepdims=True)
    mean_a = total(sum_a) / samples
    mean_r = mean_a + total(sum_v) / samples
    span = 4 * SIDE
    mid_a = jnp.broadcast_to(mean_a, (8, span))
    mid_r = jnp.broadcast_to(mean_r, (8, span))

    def squares(i, sums):
        sq_a, sq_r = sums
        for t in range(0, steps, span):
            here = (pl.ds(pl.multiple_of(i * 8, 8), 8), pl.ds(t, span))
            a = at[here]
            dev_a = a - mid_a
            dev_r = (a + vt[here]) - mid_r
            sq_a = sq_a + dev_a * dev_a
            sq_r = sq_r + dev_r * dev_r
        return sq_a, sq_r

    zero = jnp.zeros((8, span), jnp.float32)
    sq_a, sq_r = lax.fori_loop(0, envs // 8, squares, (zero, zero))
    lane = (1, SIDE)
    is_a = lax.broadcasted_iota(jnp.int32, lane, 1) < SIDE // 2

    def both(a, r):
        return jnp.where(is_a, jnp.broadcast_to(a, lane), jnp.broadcast_to(r, lane))

    st_one[0:1, :] = both(mean_a, mean_r)
    st_one[1:2, :] = both(total(sq_a) / samples, total(sq_r) / samples)
    env_stats[my_env] = st_one[...]

    for mate in mates:
        pltpu.make_async_remote_copy(
            src_ref=st_one, dst_ref=env_stats.at[my_env], send_sem=send_env, recv_sem=recv_env,
            device_id={"env": mate}, device_id_type=MESH,
        ).start()
    def advantage_sends(chunks):
        def body(middle, reach, inside, along, across):
            for c in chunks:
                for d in inside + along + across:
                    if not (middle and d in across and c >= CHUNKS - HELD):
                        send_advantages(c, d)

        by_role(body)

    advantage_sends((0, 1))
    wait_all(env_stats.at[pl.ds(0, m - 1)], recv_env)
    mean, var = combine([env_stats[q] for q in range(m)])
    st_two[0:1, :] = mean
    st_two[1:2, :] = var
    tm_stats[me] = st_two[...]
    for peer in peers:
        pltpu.make_async_remote_copy(
            src_ref=st_two, dst_ref=tm_stats.at[me], send_sem=send_tm, recv_sem=recv_tm,
            device_id={"tm": peer}, device_id_type=MESH,
        ).start()
    advantage_sends(range(2, CHUNKS))

    wait_all(tm_stats.at[pl.ds(0, n - 1)], recv_tm)
    mean, var = combine([tm_stats[q] for q in range(n)])
    scale = lax.rsqrt(var + 1e-05)
    wide = (8, part)
    mid_a, mid_r, scale_a, scale_r = (
        jnp.broadcast_to(x[0:1, i : i + 1], wide) for x in (mean, scale) for i in (0, SIDE // 2)
    )

    def normalize(read_a, read_v, first):
        for r in range(0, rows, 8):
            here = (pl.ds(r, 8), pl.ds(first, part))
            a = read_a(r)
            v = read_v(r)
            out_a[here] = (a - mid_a) * scale_a
            out_v[here] = ((a + v) - mid_r) * scale_r

    def own(c, unused):
        def read(source):
            return lambda r: source[
                pl.ds(pl.multiple_of(me * rows + r, 8), 8),
                pl.ds(pl.multiple_of(c * part, SIDE), part),
            ]
        normalize(read(at), read(vt), pl.multiple_of(me * steps + c * part, SIDE))
        return unused

    lax.fori_loop(0, CHUNKS, own, 0)

    def landed(place, c):
        if c == 0:
            wait_all(out_v.at[:, pl.ds(0, steps)], recv_v.at[place])
        wait_all(out_a.at[:, pl.ds(0, part)], recv_a.at[place * CHUNKS + c])

    def arrived(place, c, waited):
        first = pl.multiple_of(peers[place] * steps + c * part, SIDE)
        if not waited:
            landed(place, c)
        read = lambda source: lambda r: source[pl.ds(r, 8), pl.ds(first, part)]
        normalize(read(out_a), read(out_v), first)

    unused_reach, inside, along, across = plan(n, True)
    far = [d for d in across if lines // 2 <= d // side < lines - 1]
    for c in range(HELD_TILL):
        for d in far:
            landed(d - 1, c)

    @pl.when(middle)
    def unused_held():
        for c in range(CHUNKS - HELD, CHUNKS):
            for d in across[::-1]:
                send_advantages(c, d)

    for c in range(CHUNKS):
        for d in inside + along + across[::-1]:
            arrived(d - 1, c, d in far and c < HELD_TILL)

    wait_all(others, send_sum)

    @pl.when(later)
    def unused_crossed():
        crossing.wait_send()

    wait_all(env_stats.at[pl.ds(0, m - 1)], send_env)
    wait_all(tm_stats.at[pl.ds(0, n - 1)], send_tm)
    for which, source in enumerate((vt, at)):
        wait_all(source.at[pl.ds(0, (n - 1) * rows)], send_big.at[which])


def drain_kernel(a, v, out_a, out_v, sems):
    part = a.shape[0] // PIECES
    copies = [
        pltpu.make_async_copy(source.at[pl.ds(i * part, part)], target.at[pl.ds(i * part, part)], sems.at[k, i])
        for i in range(PIECES)
        for k, (source, target) in enumerate(((a, out_a), (v, out_v)))
    ]
    for copy in copies:
        copy.start()
    for copy in copies:
        copy.wait()


def drain(a, v):
    shape = jax.ShapeDtypeStruct(a.shape, a.dtype)
    local = pl.BlockSpec(memory_space=pltpu.VMEM)
    remote = pl.BlockSpec(memory_space=pltpu.HBM)
    return pl.pallas_call(
        drain_kernel,
        out_shape=(shape, shape),
        in_specs=(local, local),
        out_specs=(remote, remote),
        scratch_shapes=[pltpu.SemaphoreType.DMA((2, PIECES))],
        compiler_params=pltpu.CompilerParams(vmem_limit_bytes=1024 * 1024),
    )(a, v)


def shards(rewards, values, last_value, done_steps, horizon_offset, discount_rate, trace_rate):
    steps, envs = rewards.shape
    n, m = lax.axis_size("tm"), lax.axis_size("env")
    rows = envs // n
    horizon = steps * n // 2
    whole = pltpu.VMEM((rows, steps * n), jnp.float32)
    kernel = functools.partial(exchange, n, m, horizon, float(steps * envs))
    remote = pl.BlockSpec(memory_space=pltpu.HBM)
    local = pl.BlockSpec(memory_space=pltpu.VMEM)
    f32 = jnp.float32
    dma = pltpu.SemaphoreType.DMA
    a, v = pl.pallas_call(
        kernel,
        out_shape=(whole, whole),
        in_specs=[remote] * 7,
        out_specs=(local, local),
        scratch_shapes=[
            pltpu.VMEM((1, envs), f32),
            pltpu.VMEM(done_steps.shape[::-1], jnp.int32),
            pltpu.VMEM((1, envs), jnp.int32),
            pltpu.VMEM((1, envs), f32),
            pltpu.VMEM((1, envs), f32),
            pltpu.VMEM((steps, envs), f32),
            pltpu.VMEM((steps, envs), f32),
            pltpu.VMEM((steps, envs), f32),
            pltpu.VMEM((envs, steps), f32),
            pltpu.VMEM((envs, steps), f32),
            pltpu.VMEM((8, envs), f32),
            pltpu.VMEM((n // 2, 8, envs), f32),
            pltpu.VMEM((2, envs), f32),
            pltpu.VMEM((2, envs), f32),
            pltpu.VMEM((2, SIDE), f32),
            pltpu.VMEM((m, 2, SIDE), f32),
            pltpu.VMEM((2, SIDE), f32),
            pltpu.VMEM((n, 2, SIDE), f32),
            dma((5,)), dma, dma((CHUNKS + 1,)), dma((2,)), dma((n - 1,)), dma(((n - 1) * CHUNKS,)), dma, dma,
            dma, dma, dma, dma, dma, dma, pltpu.SemaphoreType.REGULAR((n,)),
        ],
        compiler_params=pltpu.CompilerParams(
            collective_id=0, has_side_effects=True, vmem_limit_bytes=55 * 1024 * 1024
        ),
    )(
        rewards,
        values,
        last_value[None, :],
        done_steps.T,
        horizon_offset[None, :],
        discount_rate[None, :],
        trace_rate[None, :],
    )
    return drain(a, v)


def solution(mesh):
    in_specs = (
        P("tm", "env"),
        P("tm", "env"),
        P("env"),
        P("env", None),
        P("env"),
        P("env"),
        P("env"),
    )
    out_specs = (P(("env", "tm"), None), P(("env", "tm"), None))
    return jax.shard_map(shards, mesh=mesh, in_specs=in_specs, out_specs=out_specs, check_vma=False)
```

```python
import functools

import jax
import jax.numpy as jnp
from jax import lax
from jax.experimental import pallas as pl
from jax.experimental.pallas import tpu as pltpu
from jax.sharding import PartitionSpec as P

MESH = pl.DeviceIdType.MESH
CHUNKS = 4
SIDE = 128
PIECES = 4
EARLY = 2


def combine(parts):
    count = len(parts)
    means = [part[0:1] for part in parts]
    mean = functools.reduce(jnp.add, means) / count
    spread = [part[1:2] + (m - mean) * (m - mean) for part, m in zip(parts, means)]
    return mean, functools.reduce(jnp.add, spread) / count


def grid_of(n):
    side = 1 << ((n.bit_length() - 1) // 2)
    return n // side, side


def hops(n, i, j):
    side = grid_of(n)[1]
    return abs(i // side - j // side) + abs(i % side - j % side)


def plan(n, middle):
    lines, side = grid_of(n)
    mine = [i for i in range(n) if (i // side in (lines // 2 - 1, lines // 2)) == middle]
    reach = {d: max(hops(n, i, i ^ d) for i in mine) for d in range(1, n)}
    inside = [d for d in range(side, n // 2)]
    along = [d for d in range(1, side)]
    across = sorted(range(n // 2, n), key=lambda d: (d // side, -(d % side)) if middle else -d)
    return reach, inside, along, across


def exchange(
    n, m, horizon, samples,
    rewards, values, last_in, done_in, offset_in, rate_d_in, rate_t_in,
    out_a, out_v,
    last, done, offset, rate_d, rate_t,
    p_buf, v_buf, d_buf, vt, at, src, summary, border, entry, st_one, env_stats, st_two, tm_stats,
    load_small, load_r, load_v, send_big, recv_v, recv_a, send_sum, recv_sum, send_border, recv_border,
    send_env, recv_env, send_tm, recv_tm, gates,
):
    steps, envs = v_buf.shape
    rows = envs // n
    part = steps // CHUNKS
    me = lax.axis_index("tm")
    my_env = lax.axis_index("env")
    lines, side = grid_of(n)
    line, spot = me // side, lax.rem(me, side)
    middle = jnp.logical_or(line == lines // 2 - 1, line == lines // 2)
    peers = [jnp.bitwise_xor(me, d) for d in range(1, n)]
    mates = [lax.rem(my_env + d, m) for d in range(1, m)]

    neighbours = [
        (line > 0, me - side),
        (line < lines - 1, me + side),
        (spot > 0, me - 1),
        (spot < side - 1, me + 1),
    ]
    near = functools.reduce(jnp.add, [there.astype(jnp.int32) for there, unused in neighbours])

    def announce(sem):
        for there, peer in neighbours:
            @pl.when(there)
            def unused_tell():
                pl.semaphore_signal(sem, inc=1, device_id={"tm": peer}, device_id_type=MESH)

    barrier = pltpu.get_barrier_semaphore()
    for mate in mates:
        pl.semaphore_signal(barrier, inc=1, device_id={"env": mate}, device_id_type=MESH)
    announce(barrier)

    cuts = [(0, SIDE), (SIDE, part - SIDE)] + [(c * part, part) for c in range(1, CHUNKS)]
    loads_v = [
        pltpu.make_async_copy(
            values.at[pl.ds(t, size)], v_buf.at[pl.ds(t, size)], load_v.at[c]
        )
        for c, (t, size) in enumerate(cuts)
    ]
    loading_r = pltpu.make_async_copy(rewards, p_buf, load_r)
    loads_small = [
        pltpu.make_async_copy(source, target, load_small.at[i])
        for i, (source, target) in enumerate(
            ((done_in, done), (offset_in, offset), (rate_d_in, rate_d), (rate_t_in, rate_t), (last_in, last))
        )
    ]
    for load in loads_v + loads_small + [loading_r]:
        load.start()

    def send_part(which, source, target, sem, first, width, d):
        peer = peers[d - 1]
        pltpu.make_async_remote_copy(
            src_ref=source.at[
                pl.ds(pl.multiple_of(peer * rows, 8), rows), pl.ds(first, width)
            ],
            dst_ref=target.at[
                pl.ds(0, rows), pl.ds(pl.multiple_of(me * steps + first, SIDE), width)
            ],
            send_sem=send_big.at[which],
            recv_sem=sem,
            device_id={"tm": peer},
            device_id_type=MESH,
        ).start()

    def send_values(first, width, d):
        send_part(0, vt, out_v, recv_v.at[d - 1], first, width, d)

    def send_advantages(c, d):
        send_part(1, at, out_a, recv_a.at[(d - 1) * CHUNKS + c], c * part, part, d)

    def by_role(body):
        @pl.when(middle)
        def unused_middle():
            body(True, *plan(n, True))

        @pl.when(jnp.logical_not(middle))
        def unused_end():
            body(False, *plan(n, False))

    def turn_values(first, width):
        def body(b, unused):
            t = pl.multiple_of(first + b * SIDE, SIDE)
            for e in range(0, envs, SIDE):
                vt[pl.ds(e, SIDE), pl.ds(t, SIDE)] = v_buf[pl.ds(t, SIDE), pl.ds(e, SIDE)].T
            return unused

        lax.fori_loop(0, width // SIDE, body, 0)

    for load, (t, size) in zip(loads_v[:2], cuts[:2]):
        load.wait()
        turn_values(t, size)
    pl.semaphore_wait(barrier, near + m - 1)

    farthest = lines + side - 2
    for k in range(1, farthest + 1):
        if k > 1:
            pl.semaphore_wait(gates.at[k - 2], near)
        if k < farthest:
            announce(gates.at[k - 1])

        def first_sends(middle, reach, inside, along, across):
            for d in inside + (across if middle else []) + along:
                if reach[d] == k:
                    for t, size in cuts[:2]:
                        send_values(t, size, d)

        by_role(first_sends)
        if k == 1:
            loads_v[2].wait()
            turn_values(part, part)

    def second_sends(middle, reach, inside, along, across):
        for d in across[:EARLY] if middle else inside + along:
            send_values(part, part, d)

    by_role(second_sends)
    for c in range(2, CHUNKS):
        loads_v[c + 1].wait()
    loading_r.wait()
    for load in loads_small:
        load.wait()

    discount = jnp.exp(-rate_d[...])
    retention = discount * jnp.exp(-rate_t[...])
    first = me * steps
    wide = (8, envs)
    ends = [jnp.broadcast_to(done[j : j + 1, :] - first, wide) for j in range(done.shape[0])]
    resets = [
        jnp.broadcast_to(k * horizon - 1 - first - offset[...], wide)
        for k in (1, 2)
    ]
    disc = jnp.broadcast_to(discount, wide)
    keep = jnp.broadcast_to(retention, wide)
    row = lax.broadcasted_iota(jnp.int32, wide, 0)

    def tile(k, later, final):
        v_later, a_later, d_later = later
        at_rows = pl.ds(pl.multiple_of(k * 8, 8), 8)
        v = v_buf[at_rows, :]
        r = p_buf[at_rows, :]
        moment = row + k * 8
        finished = functools.reduce(jnp.logical_or, [moment == e for e in ends])
        stopped = functools.reduce(jnp.logical_or, [moment == e for e in resets], finished)
        reach = jnp.where(finished, 0.0, disc)
        decay = jnp.where(stopped, 0.0, keep)
        v_up = pltpu.roll(v, 7, 0)
        if final:
            src[3:4, :] = reach[7:8, :]
            src[4:5, :] = decay[7:8, :]
            td = r + jnp.where(row == 7, 0.0, reach * v_up) - v
            decay = jnp.where(row == 7, 1.0, decay)
        else:
            td = r + reach * jnp.where(row == 7, v_later, v_up) - v
        for s in (1, 2, 4):
            inside = row < 8 - s
            td_up = jnp.where(inside, pltpu.roll(td, 8 - s, 0), 0.0)
            decay_up = jnp.where(inside, pltpu.roll(decay, 8 - s, 0), 1.0)
            td = td + decay * td_up
            decay = decay * decay_up
        if not final:
            td = td + decay * a_later
            decay = decay * d_later
        p_buf[at_rows, :] = td
        d_buf[at_rows, :] = decay
        return (
            v_up,
            jnp.broadcast_to(td[0:1, :], wide),
            jnp.broadcast_to(decay[0:1, :], wide),
        )

    tiles = steps // 8
    state = tile(tiles - 1, (None, None, None), True)
    lax.fori_loop(0, tiles - 1, lambda i, s: tile(tiles - 2 - i, s, False), state)

    src[0:1, :] = p_buf[0:1, :]
    src[1:2, :] = d_buf[0:1, :]
    src[2:3, :] = v_buf[0:1, :]
    src[5:8, :] = jnp.zeros((3, envs), jnp.float32)
    half = n // 2
    place = lax.rem(me, half)
    later = me >= half
    summary[place] = src[...]
    for d in range(1, half):
        pltpu.make_async_remote_copy(
            src_ref=src, dst_ref=summary.at[place], send_sem=send_sum, recv_sem=recv_sum,
            device_id={"tm": peers[d - 1]}, device_id_type=MESH,
        ).start()

    def other_sends(middle, reach, inside, along, across):
        for c in range(CHUNKS):
            near_by = inside + along
            if c < (1 if middle else 2):
                near_by = []
            far_side = across
            if middle and c == 0:
                far_side = []
            if middle and c == 1:
                far_side = across[EARLY:]
            for d in near_by + far_side:
                if c == 0:
                    for t, size in cuts[:2]:
                        send_values(t, size, d)
                else:
                    send_values(c * part, part, d)

    def wait_all(source_like, sem):
        pltpu.make_async_copy(source_like, source_like, sem).wait()

    turn_values(2 * part, steps - 2 * part)

    @pl.when(jnp.logical_not(later))
    def unused_send_early():
        by_role(other_sends)

    others = summary.at[pl.ds(0, half - 1)]
    wait_all(others, recv_sum)

    crossing = pltpu.make_async_remote_copy(
        src_ref=border, dst_ref=entry, send_sem=send_border, recv_sem=recv_border,
        device_id={"tm": peers[half - 1]}, device_id_type=MESH,
    )

    @pl.when(later)
    def unused_last():
        entry[0:1, :] = jnp.zeros((1, envs), jnp.float32)
        entry[1:2, :] = last[...]

    @pl.when(jnp.logical_not(later))
    def unused_entry():
        crossing.wait_recv()

    a_next = entry[0:1, :]
    v_next = entry[1:2, :]
    lift = jnp.zeros((1, envs), jnp.float32)
    for p in reversed(range(half)):
        block = summary[p]
        added = block[3:4] * v_next + block[4:5] * a_next
        lift = jnp.where(place == p, added, lift)
        a_next = block[0:1] + block[1:2] * added
        v_next = block[2:3]
    border[0:1, :] = a_next
    border[1:2, :] = v_next

    @pl.when(later)
    def unused_cross():
        crossing.start()
        by_role(other_sends)

    src_lift = [jnp.broadcast_to(lift[:, e : e + SIDE], (SIDE, SIDE)) for e in range(0, envs, SIDE)]

    def fold(x):
        return jnp.sum(x.reshape(SIDE // 8, 8, SIDE), axis=0)

    def finish(b, sums):
        sum_a, sum_v = sums
        t = pl.multiple_of(b * SIDE, SIDE)
        for i, e in enumerate(range(0, envs, SIDE)):
            here = (pl.ds(t, SIDE), pl.ds(e, SIDE))
            a = p_buf[here] + d_buf[here] * src_lift[i]
            at[pl.ds(e, SIDE), pl.ds(t, SIDE)] = a.T
            sum_a = sum_a + fold(a)
            sum_v = sum_v + fold(v_buf[here])
        return sum_a, sum_v

    zero = jnp.zeros((8, SIDE), jnp.float32)
    sum_a, sum_v = lax.fori_loop(0, steps // SIDE, finish, (zero, zero))
    total = lambda x: jnp.sum(jnp.sum(x, axis=1, keepdims=True), axis=0, keepdims=True)
    mean_a = total(sum_a) / samples
    mean_r = mean_a + total(sum_v) / samples
    span = 4 * SIDE
    mid_a = jnp.broadcast_to(mean_a, (8, span))
    mid_r = jnp.broadcast_to(mean_r, (8, span))

    def squares(i, sums):
        sq_a, sq_r = sums
        for t in range(0, steps, span):
            here = (pl.ds(pl.multiple_of(i * 8, 8), 8), pl.ds(t, span))
            a = at[here]
            dev_a = a - mid_a
            dev_r = (a + vt[here]) - mid_r
            sq_a = sq_a + dev_a * dev_a
            sq_r = sq_r + dev_r * dev_r
        return sq_a, sq_r

    zero = jnp.zeros((8, span), jnp.float32)
    sq_a, sq_r = lax.fori_loop(0, envs // 8, squares, (zero, zero))
    lane = (1, SIDE)
    is_a = lax.broadcasted_iota(jnp.int32, lane, 1) < SIDE // 2

    def both(a, r):
        return jnp.where(is_a, jnp.broadcast_to(a, lane), jnp.broadcast_to(r, lane))

    st_one[0:1, :] = both(mean_a, mean_r)
    st_one[1:2, :] = both(total(sq_a) / samples, total(sq_r) / samples)
    env_stats[my_env] = st_one[...]

    for mate in mates:
        pltpu.make_async_remote_copy(
            src_ref=st_one, dst_ref=env_stats.at[my_env], send_sem=send_env, recv_sem=recv_env,
            device_id={"env": mate}, device_id_type=MESH,
        ).start()
    def advantage_sends(chunks):
        def body(middle, reach, inside, along, across):
            for c in chunks:
                for d in inside + along + across:
                    send_advantages(c, d)

        by_role(body)

    advantage_sends((0, 1))
    wait_all(env_stats.at[pl.ds(0, m - 1)], recv_env)
    mean, var = combine([env_stats[q] for q in range(m)])
    st_two[0:1, :] = mean
    st_two[1:2, :] = var
    tm_stats[me] = st_two[...]
    for peer in peers:
        pltpu.make_async_remote_copy(
            src_ref=st_two, dst_ref=tm_stats.at[me], send_sem=send_tm, recv_sem=recv_tm,
            device_id={"tm": peer}, device_id_type=MESH,
        ).start()
    advantage_sends(range(2, CHUNKS))

    wait_all(tm_stats.at[pl.ds(0, n - 1)], recv_tm)
    mean, var = combine([tm_stats[q] for q in range(n)])
    scale = lax.rsqrt(var + 1e-05)
    wide = (8, part)
    mid_a, mid_r, scale_a, scale_r = (
        jnp.broadcast_to(x[0:1, i : i + 1], wide) for x in (mean, scale) for i in (0, SIDE // 2)
    )

    def normalize(read_a, read_v, first):
        for r in range(0, rows, 8):
            here = (pl.ds(r, 8), pl.ds(first, part))
            a = read_a(r)
            v = read_v(r)
            out_a[here] = (a - mid_a) * scale_a
            out_v[here] = ((a + v) - mid_r) * scale_r

    def own(c, unused):
        def read(source):
            return lambda r: source[
                pl.ds(pl.multiple_of(me * rows + r, 8), 8),
                pl.ds(pl.multiple_of(c * part, SIDE), part),
            ]
        normalize(read(at), read(vt), pl.multiple_of(me * steps + c * part, SIDE))
        return unused

    lax.fori_loop(0, CHUNKS, own, 0)

    def arrived(place, c):
        first = pl.multiple_of(peers[place] * steps + c * part, SIDE)
        if c == 0:
            wait_all(out_v.at[:, pl.ds(0, steps)], recv_v.at[place])
        wait_all(out_a.at[:, pl.ds(0, part)], recv_a.at[place * CHUNKS + c])
        read = lambda source: lambda r: source[pl.ds(r, 8), pl.ds(first, part)]
        normalize(read(out_a), read(out_v), first)

    unused_reach, inside, along, across = plan(n, True)
    for c in range(CHUNKS):
        for d in inside + along + across:
            arrived(d - 1, c)

    wait_all(others, send_sum)

    @pl.when(later)
    def unused_crossed():
        crossing.wait_send()

    wait_all(env_stats.at[pl.ds(0, m - 1)], send_env)
    wait_all(tm_stats.at[pl.ds(0, n - 1)], send_tm)
    for which, source in enumerate((vt, at)):
        wait_all(source.at[pl.ds(0, (n - 1) * rows)], send_big.at[which])


def drain_kernel(a, v, out_a, out_v, sems):
    part = a.shape[0] // PIECES
    copies = [
        pltpu.make_async_copy(source.at[pl.ds(i * part, part)], target.at[pl.ds(i * part, part)], sems.at[k, i])
        for i in range(PIECES)
        for k, (source, target) in enumerate(((a, out_a), (v, out_v)))
    ]
    for copy in copies:
        copy.start()
    for copy in copies:
        copy.wait()


def drain(a, v):
    shape = jax.ShapeDtypeStruct(a.shape, a.dtype)
    local = pl.BlockSpec(memory_space=pltpu.VMEM)
    remote = pl.BlockSpec(memory_space=pltpu.HBM)
    return pl.pallas_call(
        drain_kernel,
        out_shape=(shape, shape),
        in_specs=(local, local),
        out_specs=(remote, remote),
        scratch_shapes=[pltpu.SemaphoreType.DMA((2, PIECES))],
        compiler_params=pltpu.CompilerParams(vmem_limit_bytes=1024 * 1024),
    )(a, v)


def shards(rewards, values, last_value, done_steps, horizon_offset, discount_rate, trace_rate):
    steps, envs = rewards.shape
    n, m = lax.axis_size("tm"), lax.axis_size("env")
    rows = envs // n
    horizon = steps * n // 2
    whole = pltpu.VMEM((rows, steps * n), jnp.float32)
    kernel = functools.partial(exchange, n, m, horizon, float(steps * envs))
    remote = pl.BlockSpec(memory_space=pltpu.HBM)
    local = pl.BlockSpec(memory_space=pltpu.VMEM)
    f32 = jnp.float32
    dma = pltpu.SemaphoreType.DMA
    a, v = pl.pallas_call(
        kernel,
        out_shape=(whole, whole),
        in_specs=[remote] * 7,
        out_specs=(local, local),
        scratch_shapes=[
            pltpu.VMEM((1, envs), f32),
            pltpu.VMEM(done_steps.shape[::-1], jnp.int32),
            pltpu.VMEM((1, envs), jnp.int32),
            pltpu.VMEM((1, envs), f32),
            pltpu.VMEM((1, envs), f32),
            pltpu.VMEM((steps, envs), f32),
            pltpu.VMEM((steps, envs), f32),
            pltpu.VMEM((steps, envs), f32),
            pltpu.VMEM((envs, steps), f32),
            pltpu.VMEM((envs, steps), f32),
            pltpu.VMEM((8, envs), f32),
            pltpu.VMEM((n // 2, 8, envs), f32),
            pltpu.VMEM((2, envs), f32),
            pltpu.VMEM((2, envs), f32),
            pltpu.VMEM((2, SIDE), f32),
            pltpu.VMEM((m, 2, SIDE), f32),
            pltpu.VMEM((2, SIDE), f32),
            pltpu.VMEM((n, 2, SIDE), f32),
            dma((5,)), dma, dma((CHUNKS + 1,)), dma((2,)), dma((n - 1,)), dma(((n - 1) * CHUNKS,)), dma, dma,
            dma, dma, dma, dma, dma, dma, pltpu.SemaphoreType.REGULAR((n,)),
        ],
        compiler_params=pltpu.CompilerParams(
            collective_id=0, has_side_effects=True, vmem_limit_bytes=55 * 1024 * 1024
        ),
    )(
        rewards,
        values,
        last_value[None, :],
        done_steps.T,
        horizon_offset[None, :],
        discount_rate[None, :],
        trace_rate[None, :],
    )
    return drain(a, v)


def solution(mesh):
    in_specs = (
        P("tm", "env"),
        P("tm", "env"),
        P("env"),
        P("env", None),
        P("env"),
        P("env"),
        P("env"),
    )
    out_specs = (P(("env", "tm"), None), P(("env", "tm"), None))
    return jax.shard_map(shards, mesh=mesh, in_specs=in_specs, out_specs=out_specs, check_vma=False)
```

```python
import functools

import jax
import jax.numpy as jnp
from jax import lax
from jax.experimental import pallas as pl
from jax.experimental.pallas import tpu as pltpu
from jax.sharding import PartitionSpec as P

MESH = pl.DeviceIdType.MESH
CHUNKS = 4
SIDE = 128
PIECES = 4
EARLY = 2


def combine(parts):
    count = len(parts)
    means = [part[0:1] for part in parts]
    mean = functools.reduce(jnp.add, means) / count
    spread = [part[1:2] + (m - mean) * (m - mean) for part, m in zip(parts, means)]
    return mean, functools.reduce(jnp.add, spread) / count


def grid_of(n):
    side = 1 << ((n.bit_length() - 1) // 2)
    return n // side, side


def hops(n, i, j):
    side = grid_of(n)[1]
    return abs(i // side - j // side) + abs(i % side - j % side)


def plan(n, middle):
    lines, side = grid_of(n)
    mine = [i for i in range(n) if (i // side in (lines // 2 - 1, lines // 2)) == middle]
    reach = {d: max(hops(n, i, i ^ d) for i in mine) for d in range(1, n)}
    inside = [d for d in range(side, n // 2)]
    along = [d for d in range(1, side)]
    across = sorted(range(n // 2, n), key=lambda d: (d // side, -(d % side)) if middle else -d)
    return reach, inside, along, across


def exchange(
    n, m, horizon, samples,
    rewards, values, last_in, done_in, offset_in, rate_d_in, rate_t_in,
    out_a, out_v,
    last, done, offset, rate_d, rate_t,
    p_buf, v_buf, d_buf, vt, at, src, summary, border, entry, st_one, env_stats, st_two, tm_stats,
    load_small, load_r, load_v, send_big, recv_v, recv_a, send_sum, recv_sum, send_border, recv_border,
    send_env, recv_env, send_tm, recv_tm, gates,
):
    steps, envs = v_buf.shape
    rows = envs // n
    part = steps // CHUNKS
    me = lax.axis_index("tm")
    my_env = lax.axis_index("env")
    lines, side = grid_of(n)
    line, spot = me // side, lax.rem(me, side)
    middle = jnp.logical_or(line == lines // 2 - 1, line == lines // 2)
    peers = [jnp.bitwise_xor(me, d) for d in range(1, n)]
    mates = [lax.rem(my_env + d, m) for d in range(1, m)]

    neighbours = [
        (line > 0, me - side),
        (line < lines - 1, me + side),
        (spot > 0, me - 1),
        (spot < side - 1, me + 1),
    ]
    near = functools.reduce(jnp.add, [there.astype(jnp.int32) for there, unused in neighbours])

    def announce(sem):
        for there, peer in neighbours:
            @pl.when(there)
            def unused_tell():
                pl.semaphore_signal(sem, inc=1, device_id={"tm": peer}, device_id_type=MESH)

    barrier = pltpu.get_barrier_semaphore()
    for mate in mates:
        pl.semaphore_signal(barrier, inc=1, device_id={"env": mate}, device_id_type=MESH)
    announce(barrier)

    cuts = [(0, SIDE), (SIDE, part - SIDE)] + [(c * part, part) for c in range(1, CHUNKS)]
    loads_v = [
        pltpu.make_async_copy(
            values.at[pl.ds(t, size)], v_buf.at[pl.ds(t, size)], load_v.at[c]
        )
        for c, (t, size) in enumerate(cuts)
    ]
    loading_r = pltpu.make_async_copy(rewards, p_buf, load_r)
    loads_small = [
        pltpu.make_async_copy(source, target, load_small.at[i])
        for i, (source, target) in enumerate(
            ((done_in, done), (offset_in, offset), (rate_d_in, rate_d), (rate_t_in, rate_t), (last_in, last))
        )
    ]
    for load in loads_v + loads_small + [loading_r]:
        load.start()

    def send_part(which, source, target, sem, first, width, d):
        peer = peers[d - 1]
        pltpu.make_async_remote_copy(
            src_ref=source.at[
                pl.ds(pl.multiple_of(peer * rows, 8), rows), pl.ds(first, width)
            ],
            dst_ref=target.at[
                pl.ds(0, rows), pl.ds(pl.multiple_of(me * steps + first, SIDE), width)
            ],
            send_sem=send_big.at[which],
            recv_sem=sem,
            device_id={"tm": peer},
            device_id_type=MESH,
        ).start()

    def send_values(first, width, d):
        send_part(0, vt, out_v, recv_v.at[d - 1], first, width, d)

    def send_advantages(c, d):
        send_part(1, at, out_a, recv_a.at[(d - 1) * CHUNKS + c], c * part, part, d)

    def by_role(body):
        @pl.when(middle)
        def unused_middle():
            body(True, *plan(n, True))

        @pl.when(jnp.logical_not(middle))
        def unused_end():
            body(False, *plan(n, False))

    def turn_values(first, width):
        def body(b, unused):
            t = pl.multiple_of(first + b * SIDE, SIDE)
            for e in range(0, envs, SIDE):
                vt[pl.ds(e, SIDE), pl.ds(t, SIDE)] = v_buf[pl.ds(t, SIDE), pl.ds(e, SIDE)].T
            return unused

        lax.fori_loop(0, width // SIDE, body, 0)

    for load, (t, size) in zip(loads_v[:2], cuts[:2]):
        load.wait()
        turn_values(t, size)
    pl.semaphore_wait(barrier, near + m - 1)

    farthest = lines + side - 2
    for k in range(1, farthest + 1):
        if k > 1:
            pl.semaphore_wait(gates.at[k - 2], near)
        if k < farthest:
            announce(gates.at[k - 1])

        def first_sends(middle, reach, inside, along, across):
            for d in inside + (across if middle else []) + along:
                if reach[d] == k:
                    for t, size in cuts[:2]:
                        send_values(t, size, d)

        by_role(first_sends)
        if k == 1:
            loads_v[2].wait()
            turn_values(part, part)

    def second_sends(middle, reach, inside, along, across):
        for d in across[:EARLY] if middle else inside + along:
            send_values(part, part, d)

    by_role(second_sends)
    for c in range(2, CHUNKS):
        loads_v[c + 1].wait()
    loading_r.wait()
    for load in loads_small:
        load.wait()

    discount = jnp.exp(-rate_d[...])
    retention = discount * jnp.exp(-rate_t[...])
    first = me * steps
    wide = (8, envs)
    ends = [jnp.broadcast_to(done[j : j + 1, :] - first, wide) for j in range(done.shape[0])]
    resets = [
        jnp.broadcast_to(k * horizon - 1 - first - offset[...], wide)
        for k in (1, 2)
    ]
    disc = jnp.broadcast_to(discount, wide)
    keep = jnp.broadcast_to(retention, wide)
    row = lax.broadcasted_iota(jnp.int32, wide, 0)

    def tile(k, later, final):
        v_later, a_later, d_later = later
        at_rows = pl.ds(pl.multiple_of(k * 8, 8), 8)
        v = v_buf[at_rows, :]
        r = p_buf[at_rows, :]
        moment = row + k * 8
        finished = functools.reduce(jnp.logical_or, [moment == e for e in ends])
        stopped = functools.reduce(jnp.logical_or, [moment == e for e in resets], finished)
        reach = jnp.where(finished, 0.0, disc)
        decay = jnp.where(stopped, 0.0, keep)
        v_up = pltpu.roll(v, 7, 0)
        if final:
            src[3:4, :] = reach[7:8, :]
            src[4:5, :] = decay[7:8, :]
            td = r + jnp.where(row == 7, 0.0, reach * v_up) - v
            decay = jnp.where(row == 7, 1.0, decay)
        else:
            td = r + reach * jnp.where(row == 7, v_later, v_up) - v
        for s in (1, 2, 4):
            inside = row < 8 - s
            td_up = jnp.where(inside, pltpu.roll(td, 8 - s, 0), 0.0)
            decay_up = jnp.where(inside, pltpu.roll(decay, 8 - s, 0), 1.0)
            td = td + decay * td_up
            decay = decay * decay_up
        if not final:
            td = td + decay * a_later
            decay = decay * d_later
        p_buf[at_rows, :] = td
        d_buf[at_rows, :] = decay
        return (
            v_up,
            jnp.broadcast_to(td[0:1, :], wide),
            jnp.broadcast_to(decay[0:1, :], wide),
        )

    tiles = steps // 8
    state = tile(tiles - 1, (None, None, None), True)
    lax.fori_loop(0, tiles - 1, lambda i, s: tile(tiles - 2 - i, s, False), state)

    src[0:1, :] = p_buf[0:1, :]
    src[1:2, :] = d_buf[0:1, :]
    src[2:3, :] = v_buf[0:1, :]
    src[5:8, :] = jnp.zeros((3, envs), jnp.float32)
    half = n // 2
    place = lax.rem(me, half)
    later = me >= half
    summary[place] = src[...]
    for d in range(1, half):
        pltpu.make_async_remote_copy(
            src_ref=src, dst_ref=summary.at[place], send_sem=send_sum, recv_sem=recv_sum,
            device_id={"tm": peers[d - 1]}, device_id_type=MESH,
        ).start()

    def other_sends(middle, reach, inside, along, across):
        for c in range(CHUNKS):
            near_by = inside + along
            if c < (1 if middle else 2):
                near_by = []
            far_side = across
            if middle and c == 0:
                far_side = []
            if middle and c == 1:
                far_side = across[EARLY:]
            for d in near_by + far_side:
                if c == 0:
                    for t, size in cuts[:2]:
                        send_values(t, size, d)
                elif c == 1:
                    send_values(part, part, d)
                elif c == 2:
                    send_values(c * part, (CHUNKS - c) * part, d)

    def wait_all(source_like, sem):
        pltpu.make_async_copy(source_like, source_like, sem).wait()

    turn_values(2 * part, steps - 2 * part)

    @pl.when(jnp.logical_not(later))
    def unused_send_early():
        by_role(other_sends)

    others = summary.at[pl.ds(0, half - 1)]
    wait_all(others, recv_sum)

    crossing = pltpu.make_async_remote_copy(
        src_ref=border, dst_ref=entry, send_sem=send_border, recv_sem=recv_border,
        device_id={"tm": peers[half - 1]}, device_id_type=MESH,
    )

    @pl.when(later)
    def unused_last():
        entry[0:1, :] = jnp.zeros((1, envs), jnp.float32)
        entry[1:2, :] = last[...]

    @pl.when(jnp.logical_not(later))
    def unused_entry():
        crossing.wait_recv()

    a_next = entry[0:1, :]
    v_next = entry[1:2, :]
    lift = jnp.zeros((1, envs), jnp.float32)
    for p in reversed(range(half)):
        block = summary[p]
        added = block[3:4] * v_next + block[4:5] * a_next
        lift = jnp.where(place == p, added, lift)
        a_next = block[0:1] + block[1:2] * added
        v_next = block[2:3]
    border[0:1, :] = a_next
    border[1:2, :] = v_next

    @pl.when(later)
    def unused_cross():
        crossing.start()
        by_role(other_sends)

    src_lift = [jnp.broadcast_to(lift[:, e : e + SIDE], (SIDE, SIDE)) for e in range(0, envs, SIDE)]

    def fold(x):
        return jnp.sum(x.reshape(SIDE // 8, 8, SIDE), axis=0)

    def finish(b, sums):
        sum_a, sum_v = sums
        t = pl.multiple_of(b * SIDE, SIDE)
        for i, e in enumerate(range(0, envs, SIDE)):
            here = (pl.ds(t, SIDE), pl.ds(e, SIDE))
            a = p_buf[here] + d_buf[here] * src_lift[i]
            at[pl.ds(e, SIDE), pl.ds(t, SIDE)] = a.T
            sum_a = sum_a + fold(a)
            sum_v = sum_v + fold(v_buf[here])
        return sum_a, sum_v

    zero = jnp.zeros((8, SIDE), jnp.float32)
    sum_a, sum_v = lax.fori_loop(0, steps // SIDE, finish, (zero, zero))
    total = lambda x: jnp.sum(jnp.sum(x, axis=1, keepdims=True), axis=0, keepdims=True)
    mean_a = total(sum_a) / samples
    mean_r = mean_a + total(sum_v) / samples
    span = 4 * SIDE
    mid_a = jnp.broadcast_to(mean_a, (8, span))
    mid_r = jnp.broadcast_to(mean_r, (8, span))

    def squares(i, sums):
        sq_a, sq_r = sums
        for t in range(0, steps, span):
            here = (pl.ds(pl.multiple_of(i * 8, 8), 8), pl.ds(t, span))
            a = at[here]
            dev_a = a - mid_a
            dev_r = (a + vt[here]) - mid_r
            sq_a = sq_a + dev_a * dev_a
            sq_r = sq_r + dev_r * dev_r
        return sq_a, sq_r

    zero = jnp.zeros((8, span), jnp.float32)
    sq_a, sq_r = lax.fori_loop(0, envs // 8, squares, (zero, zero))
    lane = (1, SIDE)
    is_a = lax.broadcasted_iota(jnp.int32, lane, 1) < SIDE // 2

    def both(a, r):
        return jnp.where(is_a, jnp.broadcast_to(a, lane), jnp.broadcast_to(r, lane))

    st_one[0:1, :] = both(mean_a, mean_r)
    st_one[1:2, :] = both(total(sq_a) / samples, total(sq_r) / samples)
    env_stats[my_env] = st_one[...]

    for mate in mates:
        pltpu.make_async_remote_copy(
            src_ref=st_one, dst_ref=env_stats.at[my_env], send_sem=send_env, recv_sem=recv_env,
            device_id={"env": mate}, device_id_type=MESH,
        ).start()
    def advantage_sends(chunks):
        def body(middle, reach, inside, along, across):
            for c in chunks:
                for d in along + inside + across:
                    send_advantages(c, d)

        by_role(body)

    advantage_sends((0, 1))
    wait_all(env_stats.at[pl.ds(0, m - 1)], recv_env)
    mean, var = combine([env_stats[q] for q in range(m)])
    st_two[0:1, :] = mean
    st_two[1:2, :] = var
    tm_stats[me] = st_two[...]
    for peer in peers:
        pltpu.make_async_remote_copy(
            src_ref=st_two, dst_ref=tm_stats.at[me], send_sem=send_tm, recv_sem=recv_tm,
            device_id={"tm": peer}, device_id_type=MESH,
        ).start()
    advantage_sends(range(2, CHUNKS))

    wait_all(tm_stats.at[pl.ds(0, n - 1)], recv_tm)
    mean, var = combine([tm_stats[q] for q in range(n)])
    scale = lax.rsqrt(var + 1e-05)
    wide = (8, part)
    mid_a, mid_r, scale_a, scale_r = (
        jnp.broadcast_to(x[0:1, i : i + 1], wide) for x in (mean, scale) for i in (0, SIDE // 2)
    )

    def normalize(read_a, read_v, first):
        for r in range(0, rows, 8):
            here = (pl.ds(r, 8), pl.ds(first, part))
            a = read_a(r)
            v = read_v(r)
            out_a[here] = (a - mid_a) * scale_a
            out_v[here] = ((a + v) - mid_r) * scale_r

    def own(c, unused):
        def read(source):
            return lambda r: source[
                pl.ds(pl.multiple_of(me * rows + r, 8), 8),
                pl.ds(pl.multiple_of(c * part, SIDE), part),
            ]
        normalize(read(at), read(vt), pl.multiple_of(me * steps + c * part, SIDE))
        return unused

    lax.fori_loop(0, CHUNKS, own, 0)

    def arrived(place, c):
        first = pl.multiple_of(peers[place] * steps + c * part, SIDE)
        if c == 0:
            wait_all(out_v.at[:, pl.ds(0, steps)], recv_v.at[place])
        wait_all(out_a.at[:, pl.ds(0, part)], recv_a.at[place * CHUNKS + c])
        read = lambda source: lambda r: source[pl.ds(r, 8), pl.ds(first, part)]
        normalize(read(out_a), read(out_v), first)

    unused_reach, inside, along, across = plan(n, True)
    for c in range(CHUNKS):
        for d in inside + along + across:
            arrived(d - 1, c)

    wait_all(others, send_sum)

    @pl.when(later)
    def unused_crossed():
        crossing.wait_send()

    wait_all(env_stats.at[pl.ds(0, m - 1)], send_env)
    wait_all(tm_stats.at[pl.ds(0, n - 1)], send_tm)
    for which, source in enumerate((vt, at)):
        wait_all(source.at[pl.ds(0, (n - 1) * rows)], send_big.at[which])


def drain_kernel(a, v, out_a, out_v, sems):
    part = a.shape[0] // PIECES
    copies = [
        pltpu.make_async_copy(source.at[pl.ds(i * part, part)], target.at[pl.ds(i * part, part)], sems.at[k, i])
        for i in range(PIECES)
        for k, (source, target) in enumerate(((a, out_a), (v, out_v)))
    ]
    for copy in copies:
        copy.start()
    for copy in copies:
        copy.wait()


def drain(a, v):
    shape = jax.ShapeDtypeStruct(a.shape, a.dtype)
    local = pl.BlockSpec(memory_space=pltpu.VMEM)
    remote = pl.BlockSpec(memory_space=pltpu.HBM)
    return pl.pallas_call(
        drain_kernel,
        out_shape=(shape, shape),
        in_specs=(local, local),
        out_specs=(remote, remote),
        scratch_shapes=[pltpu.SemaphoreType.DMA((2, PIECES))],
        compiler_params=pltpu.CompilerParams(vmem_limit_bytes=1024 * 1024),
    )(a, v)


def shards(rewards, values, last_value, done_steps, horizon_offset, discount_rate, trace_rate):
    steps, envs = rewards.shape
    n, m = lax.axis_size("tm"), lax.axis_size("env")
    rows = envs // n
    horizon = steps * n // 2
    whole = pltpu.VMEM((rows, steps * n), jnp.float32)
    kernel = functools.partial(exchange, n, m, horizon, float(steps * envs))
    remote = pl.BlockSpec(memory_space=pltpu.HBM)
    local = pl.BlockSpec(memory_space=pltpu.VMEM)
    f32 = jnp.float32
    dma = pltpu.SemaphoreType.DMA
    a, v = pl.pallas_call(
        kernel,
        out_shape=(whole, whole),
        in_specs=[remote] * 7,
        out_specs=(local, local),
        scratch_shapes=[
            pltpu.VMEM((1, envs), f32),
            pltpu.VMEM(done_steps.shape[::-1], jnp.int32),
            pltpu.VMEM((1, envs), jnp.int32),
            pltpu.VMEM((1, envs), f32),
            pltpu.VMEM((1, envs), f32),
            pltpu.VMEM((steps, envs), f32),
            pltpu.VMEM((steps, envs), f32),
            pltpu.VMEM((steps, envs), f32),
            pltpu.VMEM((envs, steps), f32),
            pltpu.VMEM((envs, steps), f32),
            pltpu.VMEM((8, envs), f32),
            pltpu.VMEM((n // 2, 8, envs), f32),
            pltpu.VMEM((2, envs), f32),
            pltpu.VMEM((2, envs), f32),
            pltpu.VMEM((2, SIDE), f32),
            pltpu.VMEM((m, 2, SIDE), f32),
            pltpu.VMEM((2, SIDE), f32),
            pltpu.VMEM((n, 2, SIDE), f32),
            dma((5,)), dma, dma((CHUNKS + 1,)), dma((2,)), dma((n - 1,)), dma(((n - 1) * CHUNKS,)), dma, dma,
            dma, dma, dma, dma, dma, dma, pltpu.SemaphoreType.REGULAR((n,)),
        ],
        compiler_params=pltpu.CompilerParams(
            collective_id=0, has_side_effects=True, vmem_limit_bytes=55 * 1024 * 1024
        ),
    )(
        rewards,
        values,
        last_value[None, :],
        done_steps.T,
        horizon_offset[None, :],
        discount_rate[None, :],
        trace_rate[None, :],
    )
    return drain(a, v)


def solution(mesh):
    in_specs = (
        P("tm", "env"),
        P("tm", "env"),
        P("env"),
        P("env", None),
        P("env"),
        P("env"),
        P("env"),
    )
    out_specs = (P(("env", "tm"), None), P(("env", "tm"), None))
    return jax.shard_map(shards, mesh=mesh, in_specs=in_specs, out_specs=out_specs, check_vma=False)
```
